16 devices in a mesh: dp: 2 (over y, z), tp: 8 (over x, core).
Axes of the slice: x: 4, y: 2, z: 1, core: 2. Of those that a mesh axis runs over, the one named last changes fastest.
The devices are a block of a 4x4x8 slice.
Arguments:
- hidden: bfloat16 [1536, 896], P('dp'), parts along dimension 0
- tokens: int32 [1536], P('dp'), parts along dimension 0
- embedding: bfloat16 [151936, 896], P('tp')
- head_w: bfloat16 [896, 151936], P(None, 'tp')
- h_norm: float32 [896], replicated
- e_norm: float32 [896], replicated
- f_norm: float32 [896], replicated
- o_norm: float32 [896], replicated
- proj_w: bfloat16 [1792, 896], P(None, 'tp')
- w_gate: bfloat16 [896, 4864], P(None, 'tp')
- w_up: bfloat16 [896, 4864], P(None, 'tp')
- w_down: bfloat16 [4864, 896], P('tp')
Outputs:
- output 1: bfloat16 [1536, 896], P('dp'), parts along dimension 0
- output 2: float32 [1536, 151936], P('dp', 'tp'), parts along dimension 0
There are 2 independent parts. The reference program is written for one: setup_inputs(seed, part) draws one part's arguments, and reference() takes and returns one part's arrays. A program takes and returns all parts, laid end to end along the dimension named above; an argument that names none is the same for every part.
All inputs are finite; a program needn't handle non-finite values.
Results may differ from the reference program's by a relative error of at most 0.0110913.
Values are sent between devices in bfloat16 or wider.
A program may use at most 768 MiB of HBM per device.

```python
import jax
import jax.numpy as jnp
from jax import lax

MODEL_DIM = 896
VOCAB_SIZE = 151936
FFN_DIM = 4864
BATCH_ROWS = 768

HOT_WIDTH = VOCAB_SIZE // 32
NORM_EPS = 1e-6


def draw_tokens(key_in):
    sub_keys = jax.random.split(key_in, 4)
    hot_starts = jax.random.randint(sub_keys[0], (2,), 0, VOCAB_SIZE - HOT_WIDTH + 1)
    choice = jax.random.randint(sub_keys[1], (BATCH_ROWS,), 0, 4)
    offsets = jax.random.randint(sub_keys[2], (BATCH_ROWS,), 0, HOT_WIDTH)
    spread = jax.random.randint(sub_keys[3], (BATCH_ROWS,), 0, VOCAB_SIZE)
    hot_ids = jnp.where(choice == 3, hot_starts[1], hot_starts[0]) + offsets
    token_ids = jnp.where(choice == 0, spread, hot_ids)
    return token_ids.at[0].set(0).at[BATCH_ROWS - 1].set(VOCAB_SIZE - 1).astype(jnp.int32)


def setup_inputs(seed: int = 0, part: int = 0) -> dict:
    root_key = jax.random.key(seed)
    part_keys = jax.random.split(jax.random.fold_in(root_key, part), 2)
    weight_keys = jax.random.split(root_key, 10)
    hidden = (2.0 * jax.random.normal(part_keys[0], (BATCH_ROWS, MODEL_DIM), jnp.float32)).astype(jnp.bfloat16)
    tokens = draw_tokens(part_keys[1])
    embedding = jax.random.normal(weight_keys[0], (VOCAB_SIZE, MODEL_DIM), jnp.float32).astype(jnp.bfloat16)
    head_w = (jax.random.normal(weight_keys[1], (MODEL_DIM, VOCAB_SIZE), jnp.float32) * (1.5 * MODEL_DIM ** -0.5)).astype(jnp.bfloat16)
    h_norm = 1.0 + 0.5 * jax.random.normal(weight_keys[2], (MODEL_DIM,), jnp.float32)
    e_norm = 1.0 + 0.5 * jax.random.normal(weight_keys[3], (MODEL_DIM,), jnp.float32)
    f_norm = 1.0 + 0.5 * jax.random.normal(weight_keys[4], (MODEL_DIM,), jnp.float32)
    o_norm = 1.0 + 0.5 * jax.random.normal(weight_keys[5], (MODEL_DIM,), jnp.float32)
    proj_w = (jax.random.normal(weight_keys[6], (2 * MODEL_DIM, MODEL_DIM), jnp.float32) * (2 * MODEL_DIM) ** -0.5).astype(jnp.bfloat16)
    w_gate = (jax.random.normal(weight_keys[7], (MODEL_DIM, FFN_DIM), jnp.float32) * MODEL_DIM ** -0.5).astype(jnp.bfloat16)
    w_up = (jax.random.normal(weight_keys[8], (MODEL_DIM, FFN_DIM), jnp.float32) * MODEL_DIM ** -0.5).astype(jnp.bfloat16)
    w_down = (jax.random.normal(weight_keys[9], (FFN_DIM, MODEL_DIM), jnp.float32) * FFN_DIM ** -0.5).astype(jnp.bfloat16)
    return {"hidden": hidden, "tokens": tokens, "embedding": embedding, "head_w": head_w, "h_norm": h_norm, "e_norm": e_norm, "f_norm": f_norm, "o_norm": o_norm, "proj_w": proj_w, "w_gate": w_gate, "w_up": w_up, "w_down": w_down}


def rms_norm(values, norm_gain):
    wide_vals = values.astype(jnp.float32)
    inv_rms = lax.rsqrt(jnp.mean(wide_vals * wide_vals, axis=-1, keepdims=True) + NORM_EPS)
    return wide_vals * inv_rms * norm_gain


def reference(hidden, tokens, embedding, head_w, h_norm, e_norm, f_norm, o_norm, proj_w, w_gate, w_up, w_down):
    emb_rows = jnp.take(embedding, tokens, axis=0)
    joined = jnp.concatenate([rms_norm(hidden, h_norm), rms_norm(emb_rows, e_norm)], axis=-1).astype(jnp.bfloat16)
    proj_full = jnp.dot(joined, proj_w, preferred_element_type=jnp.float32).astype(jnp.bfloat16)
    normed = rms_norm(proj_full, f_norm).astype(jnp.bfloat16)
    gate_val = jnp.dot(normed, w_gate, preferred_element_type=jnp.float32)
    up_val = jnp.dot(normed, w_up, preferred_element_type=jnp.float32)
    act_val = (jax.nn.silu(gate_val) * up_val).astype(jnp.bfloat16)
    down_val = jnp.dot(act_val, w_down, preferred_element_type=jnp.float32)
    new_u = (proj_full.astype(jnp.float32) + down_val).astype(jnp.bfloat16)
    out_norm = rms_norm(new_u, o_norm).astype(jnp.bfloat16)
    logits = jnp.dot(out_norm, head_w, preferred_element_type=jnp.float32)
    log_total = jax.nn.logsumexp(logits, axis=-1, keepdims=True)
    return new_u, logits - log_total
```

```python
import functools

import jax
import jax.numpy as jnp
from jax import lax
from jax.experimental import pallas as pl
from jax.experimental.pallas import tpu as pltpu
from jax.sharding import PartitionSpec as P

NORM_EPS = 1e-6
SLAB = 8
GROUP = 32
VOCAB_TILE = 528
F32 = jnp.float32
BF16 = jnp.bfloat16
MESH = pl.DeviceIdType.MESH


def gather_kernel(base_ref, want_ref, table_ref, out_ref, slabs, sems):
    groups = out_ref.shape[0] // GROUP
    span = GROUP * SLAB

    def issue(group, carry):
        for lane in range(GROUP):
            row = group * GROUP + lane
            base = pl.multiple_of(base_ref[row], SLAB)
            pltpu.make_async_copy(
                table_ref.at[pl.ds(base, SLAB), :],
                slabs.at[pl.ds(pl.multiple_of(row * SLAB, SLAB), SLAB), :],
                sems.at[group],
            ).start()
        return carry

    lax.fori_loop(0, groups, issue, 0)

    def select(group, carry):
        block = pl.ds(pl.multiple_of(group * span, span), span)
        rows = pl.ds(pl.multiple_of(group * GROUP, GROUP), GROUP)
        pltpu.make_async_copy(table_ref.at[pl.ds(0, span), :], slabs.at[block, :], sems.at[group]).wait()
        lanes = lax.broadcasted_iota(jnp.int32, (GROUP, span), 1)
        hot = jnp.where(want_ref[rows, :] == lanes, 1.0, 0.0).astype(BF16)
        out_ref[rows, :] = jnp.dot(hot, slabs[block, :], preferred_element_type=F32).astype(BF16)
        return carry

    lax.fori_loop(0, groups, select, 0)


def gather_rows(embedding, local_ids, owned):
    rows, dim = local_ids.shape[0], embedding.shape[1]
    spread = jnp.arange(rows, dtype=jnp.int32)
    ids = jnp.where(owned, local_ids, spread * SLAB % embedding.shape[0])
    place = spread % GROUP
    want = jnp.where(owned, place * SLAB + ids % SLAB, -1)[:, None]
    return pl.pallas_call(
        gather_kernel,
        out_shape=jax.ShapeDtypeStruct((rows, dim), BF16),
        in_specs=[
            pl.BlockSpec(memory_space=pltpu.SMEM),
            pl.BlockSpec(memory_space=pltpu.VMEM),
            pl.BlockSpec(memory_space=pl.ANY),
        ],
        out_specs=pl.BlockSpec(memory_space=pltpu.VMEM),
        scratch_shapes=[
            pltpu.VMEM((rows * SLAB, dim), BF16),
            pltpu.SemaphoreType.DMA((rows // GROUP,)),
        ],
        compiler_params=pltpu.CompilerParams(vmem_limit_bytes=24 << 20),
        name="gather_rows",
    )(ids // SLAB * SLAB, want, embedding)


def gain_row(gains, index):
    packed = gains[...]
    count = packed.shape[0] // 4
    return jnp.concatenate([packed[index * count + j : index * count + j + 1, :] for j in range(count)], axis=1)


def column_of(gain):
    return jnp.broadcast_to(gain, (128, gain.shape[1])).T


def norm_columns(src_ref, dst_ref, gain):
    gain = column_of(gain)
    dim, tokens = src_ref.shape
    for start in range(0, tokens, 128):
        lanes = pl.ds(start, 128)
        wide = src_ref[:, lanes].astype(F32)
        inv_rms = lax.rsqrt(jnp.sum(wide * wide, axis=0, keepdims=True) / dim + NORM_EPS)
        dst_ref[:, lanes] = (wide * inv_rms * gain).astype(dst_ref.dtype)


def norm_rows(wide, gain):
    inv_rms = lax.rsqrt(jnp.mean(wide * wide, axis=-1, keepdims=True) + NORM_EPS)
    return (wide * inv_rms * gain).astype(BF16)


def mix_kernel(
    n_tp,
    hidden_ref,
    picked_ref,
    gains,
    proj_t,
    gate_t,
    up_t,
    down,
    u_ref,
    o_ref,
    h_normed,
    e_full,
    p_full,
    n_full,
    a_full,
    u_full,
    comb_e,
    pair_e,
    far_e,
    part_d,
    pair_d,
    far_d,
    send_rs,
    recv_rs,
    send_ag,
    recv_ag,
):
    me = lax.axis_index("tp")
    chips = n_tp // 2
    chip, core = me // 2, me % 2
    partner = chip * 2 + 1 - core
    far = [lax.rem(chip + k, chips) for k in range(chips)]
    back = [lax.rem(chip + chips - k, chips) for k in range(chips)]
    tokens, dim = hidden_ref.shape
    t_rows = tokens // n_tp
    f_rows = proj_t.shape[0]

    barrier = pltpu.get_barrier_semaphore()
    for peer in [partner] + [far[k] * 2 + core for k in range(1, chips)]:
        pl.semaphore_signal(barrier, inc=1, device_id={"tp": peer}, device_id_type=MESH)
    pl.semaphore_wait(barrier, chips)

    def push(src, dst, send_sem, recv_sem, device):
        copy = pltpu.make_async_remote_copy(
            src_ref=src, dst_ref=dst, send_sem=send_sem, recv_sem=recv_sem, device_id={"tp": device}, device_id_type=MESH
        )
        copy.start()
        return copy

    def rows_of(device, size):
        return pl.ds(pl.multiple_of(device * size, 16), size)

    def pair_send(src, size, landing, stage):
        return [
            push(
                src.at[rows_of(c * 2 + 1 - core, size), :],
                landing.at[c],
                send_rs.at[stage, c],
                recv_rs.at[stage, c],
                partner,
            )
            for c in range(chips)
        ]

    def far_send(src, landing, k, stage):
        return push(src, landing.at[k - 1], send_rs.at[stage, k], recv_rs.at[stage, k], far[k] * 2 + core)

    def all_gather(full, size, stage):
        own = full.at[rows_of(me, size), :]
        sends = {}
        for k in [2, 1, 3]:
            sends[k] = push(own, own, send_ag.at[stage, k], recv_ag.at[stage, k], far[k] * 2 + core)
        near = push(own, own, send_ag.at[stage, 0], recv_ag.at[stage, 0], partner)
        passed = []
        for k in [1, 3, 2]:
            sends[k].wait_recv()
            block = full.at[rows_of(back[k] * 2 + core, size), :]
            passed.append(push(block, block, send_ag.at[stage, chips + k], recv_ag.at[stage, chips + k], partner))
        near.wait_recv()
        for copy in passed:
            copy.wait_recv()
        for copy in [near] + passed + list(sends.values()):
            copy.wait_send()

    e_pair = pair_send(picked_ref, t_rows, pair_e, 0)

    def norm_hidden(step, carry):
        rows = pl.ds(pl.multiple_of(step * t_rows, 16), t_rows)
        h_normed[rows, :] = norm_rows(hidden_ref[rows, :].astype(F32), gain_row(gains, 0))
        return carry

    e_far = {}
    for k in [2, 1, 3, 0]:
        c = far[k]
        for copy in [e_pair] if k == 2 else []:
            for one in copy:
                one.wait()
        comb_e[k] = picked_ref[rows_of(c * 2 + core, t_rows), :] + pair_e[c]
        if k:
            e_far[k] = far_send(comb_e.at[k], far_e, k, 1)
    lax.fori_loop(0, n_tp, norm_hidden, 0)
    total = comb_e[0]
    for k in [1, 3, 2]:
        e_far[k].wait()
        total = total + far_e[k - 1]
    e_full[rows_of(me, t_rows), :] = norm_rows(total.astype(F32), gain_row(gains, 1))
    all_gather(e_full, t_rows, 0)

    contract_last = (((1,), (1,)), ((), ()))
    p_own = lax.dot_general(proj_t[:, :dim], h_normed[...], contract_last, preferred_element_type=F32)
    p_own = p_own + lax.dot_general(proj_t[:, dim:], e_full[...], contract_last, preferred_element_type=F32)
    p_full[rows_of(me, f_rows), :] = p_own.astype(BF16)
    all_gather(p_full, f_rows, 1)

    norm_columns(p_full, n_full, gain_row(gains, 2))
    for start in range(0, tokens, 256):
        lanes = pl.ds(start, 256)
        gate_val = jnp.dot(gate_t[...], n_full[:, lanes], preferred_element_type=F32)
        up_val = jnp.dot(up_t[...], n_full[:, lanes], preferred_element_type=F32)
        a_full[:, lanes] = (gate_val * jax.nn.sigmoid(gate_val) * up_val).astype(BF16)
    contract_first = (((0,), (0,)), ((), ()))
    for start in range(0, tokens, 256):
        lanes = pl.ds(start, 256)
        part_d[:, lanes] = lax.dot_general(down[...], a_full[:, lanes], contract_first, preferred_element_type=F32)

    d_pair = pair_send(part_d, f_rows, pair_d, 2)
    d_far = {}
    for one in d_pair:
        one.wait()
    for k in [2, 1, 3, 0]:
        c = far[k]
        pair_d[c] = part_d[rows_of(c * 2 + core, f_rows), :] + pair_d[c]
        if k:
            d_far[k] = far_send(pair_d.at[c], far_d, k, 3)
    summed = pair_d[chip]
    for k in [1, 3, 2]:
        d_far[k].wait()
        summed = summed + far_d[k - 1]
    own = rows_of(me, f_rows)
    u_full[own, :] = (p_full[own, :].astype(F32) + summed).astype(BF16)
    all_gather(u_full, f_rows, 2)

    norm_columns(u_full, o_ref, gain_row(gains, 3))
    for start in range(0, tokens, 128):
        u_ref[pl.ds(start, 128), :] = u_full[:, pl.ds(start, 128)].T


def mix(n_tp, hidden, picked, gains, proj_w, w_gate, w_up, w_down):
    tokens, dim = hidden.shape
    chips = n_tp // 2
    t_rows, f_rows, ffn = tokens // n_tp, proj_w.shape[1], w_gate.shape[1]
    vmem = pl.BlockSpec(memory_space=pltpu.VMEM)
    return pl.pallas_call(
        functools.partial(mix_kernel, n_tp),
        out_shape=(jax.ShapeDtypeStruct((tokens, dim), BF16), jax.ShapeDtypeStruct((dim, tokens), BF16)),
        in_specs=[vmem] * 7,
        out_specs=(vmem, vmem),
        scratch_shapes=[
            pltpu.VMEM((tokens, dim), BF16),
            pltpu.VMEM((tokens, dim), BF16),
            pltpu.VMEM((dim, tokens), BF16),
            pltpu.VMEM((dim, tokens), BF16),
            pltpu.VMEM((ffn, tokens), BF16),
            pltpu.VMEM((dim, tokens), BF16),
            pltpu.VMEM((chips, t_rows, dim), BF16),
            pltpu.VMEM((chips, t_rows, dim), BF16),
            pltpu.VMEM((chips - 1, t_rows, dim), BF16),
            pltpu.VMEM((dim, tokens), F32),
            pltpu.VMEM((chips, f_rows, tokens), F32),
            pltpu.VMEM((chips - 1, f_rows, tokens), F32),
            pltpu.SemaphoreType.DMA((4, chips)),
            pltpu.SemaphoreType.DMA((4, chips)),
            pltpu.SemaphoreType.DMA((3, 2 * chips)),
            pltpu.SemaphoreType.DMA((3, 2 * chips)),
        ],
        compiler_params=pltpu.CompilerParams(collective_id=0, has_side_effects=True, vmem_limit_bytes=48 << 20),
        name="mix",
    )(
        hidden,
        picked,
        gains,
        proj_w.T,
        w_gate.T,
        w_up.T,
        w_down,
    )


def stats_kernel(vocab, head_ref, o_ref, max_ref, sum_ref, logits):
    step = pl.program_id(0)
    rows, tokens = logits.shape

    @pl.when(step == 0)
    def _():
        max_ref[...] = jnp.full_like(max_ref, -jnp.inf)
        sum_ref[...] = jnp.zeros_like(sum_ref)

    left = vocab - step * rows
    for start in range(0, tokens, 256):
        lanes = pl.ds(start, 256)
        z = jnp.dot(head_ref[...], o_ref[:, lanes], preferred_element_type=F32)
        index = lax.broadcasted_iota(jnp.int32, z.shape, 0)
        z = jnp.where(index < left, z, -jnp.inf).reshape(rows // 8, 8, 256)
        old = max_ref[:, lanes]
        new = jnp.maximum(old, jnp.max(z, axis=0))
        sum_ref[:, lanes] = sum_ref[:, lanes] * jnp.exp(old - new) + jnp.sum(jnp.exp(z - new[None]), axis=0)
        max_ref[:, lanes] = new


def head_stats(head_t, o_t):
    vocab, dim = head_t.shape
    tokens = o_t.shape[1]
    keep = pl.BlockSpec((8, tokens), lambda i: (0, 0))
    return pl.pallas_call(
        functools.partial(stats_kernel, vocab),
        out_shape=(jax.ShapeDtypeStruct((8, tokens), F32), jax.ShapeDtypeStruct((8, tokens), F32)),
        grid=(pl.cdiv(vocab, VOCAB_TILE),),
        in_specs=[
            pl.BlockSpec((VOCAB_TILE, dim), lambda i: (i, 0)),
            pl.BlockSpec((dim, tokens), lambda i: (0, 0)),
        ],
        out_specs=(keep, keep),
        scratch_shapes=[pltpu.VMEM((VOCAB_TILE, tokens), F32)],
        compiler_params=pltpu.CompilerParams(dimension_semantics=("arbitrary",), vmem_limit_bytes=32 << 20),
        name="head_stats",
    )(head_t, o_t)


def merge_kernel(n_tp, max_ref, sum_ref, lse_ref, mine, theirs, send_sem, recv_sem):
    me = lax.axis_index("tp")
    barrier = pltpu.get_barrier_semaphore()
    for k in range(1, n_tp):
        peer = lax.rem(me + k, n_tp)
        pl.semaphore_signal(barrier, inc=1, device_id={"tp": peer}, device_id_type=MESH)
    tokens = max_ref.shape[1]
    top = jnp.max(max_ref[...], axis=0, keepdims=True)
    scaled = jnp.sum(sum_ref[...] * jnp.exp(max_ref[...] - top), axis=0, keepdims=True)
    mine[...] = jnp.concatenate([jnp.broadcast_to(top, (8, tokens)), jnp.broadcast_to(scaled, (8, tokens))], axis=0)
    pl.semaphore_wait(barrier, n_tp - 1)
    copies = []
    for k in range(1, n_tp):
        copy = pltpu.make_async_remote_copy(
            src_ref=mine,
            dst_ref=theirs.at[k - 1],
            send_sem=send_sem.at[k - 1],
            recv_sem=recv_sem.at[k - 1],
            device_id={"tp": lax.rem(me + k, n_tp)},
            device_id_type=MESH,
        )
        copy.start()
        copies.append(copy)
    for copy in copies:
        copy.wait()
    best, total = mine[:8, :], mine[8:, :]
    for k in range(n_tp - 1):
        other, extra = theirs[k, :8, :], theirs[k, 8:, :]
        new = jnp.maximum(best, other)
        total = total * jnp.exp(best - new) + extra * jnp.exp(other - new)
        best = new
    lse_ref[...] = best + jnp.log(total)


def merge(n_tp, maxima, sums):
    tokens = maxima.shape[1]
    vmem = pl.BlockSpec(memory_space=pltpu.VMEM)
    return pl.pallas_call(
        functools.partial(merge_kernel, n_tp),
        out_shape=jax.ShapeDtypeStruct((8, tokens), F32),
        in_specs=[vmem, vmem],
        out_specs=vmem,
        scratch_shapes=[
            pltpu.VMEM((16, tokens), F32),
            pltpu.VMEM((n_tp - 1, 16, tokens), F32),
            pltpu.SemaphoreType.DMA((n_tp - 1,)),
            pltpu.SemaphoreType.DMA((n_tp - 1,)),
        ],
        compiler_params=pltpu.CompilerParams(collective_id=1, has_side_effects=True),
        name="merge",
    )(maxima, sums)


def logp_kernel(head_ref, o_ref, lse_ref, out_ref):
    tokens = o_ref.shape[1]
    for start in range(0, tokens, 256):
        lanes = pl.ds(start, 256)
        z = jnp.dot(head_ref[...], o_ref[:, lanes], preferred_element_type=F32)
        out_ref[:, lanes] = z - lse_ref[0:1, lanes]


def head_logp(head_t, o_t, lse):
    vocab, dim = head_t.shape
    tokens = o_t.shape[1]
    return pl.pallas_call(
        logp_kernel,
        out_shape=jax.ShapeDtypeStruct((vocab, tokens), F32),
        grid=(pl.cdiv(vocab, VOCAB_TILE),),
        in_specs=[
            pl.BlockSpec((VOCAB_TILE, dim), lambda i: (i, 0)),
            pl.BlockSpec((dim, tokens), lambda i: (0, 0)),
            pl.BlockSpec((8, tokens), lambda i: (0, 0)),
        ],
        out_specs=pl.BlockSpec((VOCAB_TILE, tokens), lambda i: (i, 0)),
        compiler_params=pltpu.CompilerParams(dimension_semantics=("arbitrary",), vmem_limit_bytes=32 << 20),
        name="head_logp",
    )(head_t, o_t, lse)


def solution(mesh):
    n_tp = mesh.shape["tp"]

    def draft_step(hidden, tokens, embedding, head_w, h_norm, e_norm, f_norm, o_norm, proj_w, w_gate, w_up, w_down):
        vocab_local = embedding.shape[0]
        local_ids = tokens - lax.axis_index("tp") * vocab_local
        owned = (local_ids >= 0) & (local_ids < vocab_local)
        picked = gather_rows(embedding, local_ids, owned)
        gains = jnp.concatenate([h_norm, e_norm, f_norm, o_norm]).reshape(-1, 128)
        new_u, out_t = mix(n_tp, hidden, picked, gains, proj_w, w_gate, w_up, w_down)
        head_t = head_w.T
        lse = merge(n_tp, *head_stats(head_t, out_t))
        return new_u, head_logp(head_t, out_t, lse).T

    specs_in = (
        P("dp", None), P("dp"), P("tp", None), P(None, "tp"), P(None), P(None), P(None), P(None),
        P(None, "tp"), P(None, "tp"), P(None, "tp"), P("tp", None),
    )
    specs_out = (P("dp", None), P("dp", "tp"))
    return jax.shard_map(draft_step, mesh=mesh, in_specs=specs_in, out_specs=specs_out, check_vma=False)
```

```python
import functools

import jax
import jax.numpy as jnp
from jax import lax
from jax.experimental import pallas as pl
from jax.experimental.pallas import tpu as pltpu
from jax.sharding import PartitionSpec as P

NORM_EPS = 1e-6
SLAB = 8
GROUP = 32
TILE = 1056
HALF = TILE // 2
LANES = 256
KEEPS = 6
KEEP_TILES = 12
CHUNK = 256
LOWEST = float(jnp.finfo(jnp.float32).min)
F32 = jnp.float32
BF16 = jnp.bfloat16
MESH = pl.DeviceIdType.MESH


def gather_kernel(base_ref, want_ref, table_ref, out_ref, slabs, sems):
    groups = out_ref.shape[0] // GROUP
    span = GROUP * SLAB

    def issue(group, carry):
        for lane in range(GROUP):
            row = group * GROUP + lane
            base = pl.multiple_of(base_ref[row], SLAB)
            pltpu.make_async_copy(
                table_ref.at[pl.ds(base, SLAB), :],
                slabs.at[pl.ds(pl.multiple_of(row * SLAB, SLAB), SLAB), :],
                sems.at[group],
            ).start()
        return carry

    lax.fori_loop(0, groups, issue, 0)

    def select(group, carry):
        block = pl.ds(pl.multiple_of(group * span, span), span)
        rows = pl.ds(pl.multiple_of(group * GROUP, GROUP), GROUP)
        pltpu.make_async_copy(table_ref.at[pl.ds(0, span), :], slabs.at[block, :], sems.at[group]).wait()
        lanes = lax.broadcasted_iota(jnp.int32, (GROUP, span), 1)
        hot = jnp.where(want_ref[rows, :] == lanes, 1.0, 0.0).astype(BF16)
        out_ref[rows, :] = jnp.dot(hot, slabs[block, :], preferred_element_type=F32).astype(BF16)
        return carry

    lax.fori_loop(0, groups, select, 0)


def gather_rows(embedding, local_ids, owned):
    rows, dim = local_ids.shape[0], embedding.shape[1]
    spread = jnp.arange(rows, dtype=jnp.int32)
    ids = jnp.where(owned, local_ids, spread * SLAB % embedding.shape[0])
    place = spread % GROUP
    want = jnp.where(owned, place * SLAB + ids % SLAB, -1)[:, None]
    return pl.pallas_call(
        gather_kernel,
        out_shape=jax.ShapeDtypeStruct((rows, dim), BF16),
        in_specs=[
            pl.BlockSpec(memory_space=pltpu.SMEM),
            pl.BlockSpec(memory_space=pltpu.VMEM),
            pl.BlockSpec(memory_space=pl.ANY),
        ],
        out_specs=pl.BlockSpec(memory_space=pltpu.VMEM),
        scratch_shapes=[
            pltpu.VMEM((rows * SLAB, dim), BF16),
            pltpu.SemaphoreType.DMA((rows // GROUP,)),
        ],
        compiler_params=pltpu.CompilerParams(vmem_limit_bytes=24 << 20),
        name="gather_rows",
    )(ids // SLAB * SLAB, want, embedding)


def gain_row(gains, index):
    packed = gains[...]
    count = packed.shape[0] // 4
    return jnp.concatenate([packed[index * count + j : index * count + j + 1, :] for j in range(count)], axis=1)


def column_of(gain):
    return jnp.broadcast_to(gain, (128, gain.shape[1])).T


def norm_columns(src_ref, dst_ref, gain):
    gain = column_of(gain)
    dim, tokens = src_ref.shape
    for start in range(0, tokens, 128):
        lanes = pl.ds(start, 128)
        wide = src_ref[:, lanes].astype(F32)
        inv_rms = lax.rsqrt(jnp.sum(wide * wide, axis=0, keepdims=True) / dim + NORM_EPS)
        dst_ref[:, lanes] = (wide * inv_rms * gain).astype(dst_ref.dtype)


def norm_rows(wide, gain):
    inv_rms = lax.rsqrt(jnp.mean(wide * wide, axis=-1, keepdims=True) + NORM_EPS)
    return (wide * inv_rms * gain).astype(BF16)


def mix_kernel(
    n_tp,
    hidden_ref,
    picked_ref,
    gains,
    proj_t,
    gate_t,
    up_t,
    down,
    u_ref,
    o_ref,
    h_normed,
    e_full,
    p_full,
    n_full,
    a_full,
    u_full,
    comb_e,
    pair_e,
    far_e,
    part_d,
    pair_d,
    far_d,
    send_rs,
    recv_rs,
    send_ag,
    recv_ag,
):
    me = lax.axis_index("tp")
    chips = n_tp // 2
    chip, core = me // 2, me % 2
    partner = chip * 2 + 1 - core
    far = [lax.rem(chip + k, chips) for k in range(chips)]
    back = [lax.rem(chip + chips - k, chips) for k in range(chips)]
    tokens, dim = hidden_ref.shape
    chunks = tokens // CHUNK
    t_rows = CHUNK // n_tp
    f_rows = proj_t.shape[0]
    order = [2, 1, 3]
    contract_last = (((1,), (1,)), ((), ()))
    contract_first = (((0,), (0,)), ((), ()))

    barrier = pltpu.get_barrier_semaphore()
    for peer in [partner] + [far[k] * 2 + core for k in range(1, chips)]:
        pl.semaphore_signal(barrier, inc=1, device_id={"tp": peer}, device_id_type=MESH)
    pl.semaphore_wait(barrier, chips)

    def push(src, dst, send_sem, recv_sem, device):
        copy = pltpu.make_async_remote_copy(
            src_ref=src, dst_ref=dst, send_sem=send_sem, recv_sem=recv_sem, device_id={"tp": device}, device_id_type=MESH
        )
        copy.start()
        return copy

    def token_block(chunk):
        return lambda device: (pl.ds(pl.multiple_of(chunk * CHUNK + device * t_rows, 16), t_rows), slice(None))

    def feature_block(chunk):
        return lambda device: (pl.ds(pl.multiple_of(device * f_rows, 16), f_rows), pl.ds(chunk * CHUNK, CHUNK))

    def pair_send(src, block, landing, stage, chunk):
        return [
            push(
                src.at[block(c * 2 + 1 - core)],
                landing.at[chunk, c],
                send_rs.at[stage, chunk, c],
                recv_rs.at[stage, chunk, c],
                partner,
            )
            for c in range(chips)
        ]

    def far_send(src, landing, k, stage, chunk):
        return push(
            src, landing.at[chunk, k - 1], send_rs.at[stage, chunk, k], recv_rs.at[stage, chunk, k], far[k] * 2 + core
        )

    def gather_start(full, block, stage, chunk):
        own = full.at[block(me)]
        sends = {
            k: push(own, own, send_ag.at[stage, chunk, k], recv_ag.at[stage, chunk, k], far[k] * 2 + core) for k in order
        }
        near = push(own, own, send_ag.at[stage, chunk, 0], recv_ag.at[stage, chunk, 0], partner)
        return sends, near

    def gather_pass(state, full, block, stage, chunk):
        sends, near = state
        passed = []
        for k in [1, 3, 2]:
            sends[k].wait_recv()
            view = full.at[block(back[k] * 2 + core)]
            passed.append(
                push(view, view, send_ag.at[stage, chunk, chips + k], recv_ag.at[stage, chunk, chips + k], partner)
            )
        return [near] + passed, list(sends.values())

    def gather_end(state):
        local, sends = state
        for copy in local:
            copy.wait()
        for copy in sends:
            copy.wait_send()

    live = [None] * chunks

    def e_start(chunk):
        live[chunk] = pair_send(picked_ref, token_block(chunk), pair_e, 0, chunk)

    def h_norm(chunk):
        for start in range(0, CHUNK, 64):
            rows = pl.ds(chunk * CHUNK + start, 64)
            h_normed[rows, :] = norm_rows(hidden_ref[rows, :].astype(F32), gain_row(gains, 0))

    def e_mid(chunk):
        for copy in live[chunk]:
            copy.wait()
        block, sends = token_block(chunk), {}
        for k in order + [0]:
            comb_e[chunk, k] = picked_ref[block(far[k] * 2 + core)] + pair_e[chunk, far[k]]
            if k:
                sends[k] = far_send(comb_e.at[chunk, k], far_e, k, 1, chunk)
        live[chunk] = sends

    def e_end(chunk):
        total = comb_e[chunk, 0]
        for k in [1, 3, 2]:
            live[chunk][k].wait()
            total = total + far_e[chunk, k - 1]
        block = token_block(chunk)
        e_full[block(me)] = norm_rows(total.astype(F32), gain_row(gains, 1))
        live[chunk] = gather_start(e_full, block, 0, chunk)

    def e_pass(chunk):
        live[chunk] = gather_pass(live[chunk], e_full, token_block(chunk), 0, chunk)

    def project(chunk):
        gather_end(live[chunk])
        rows, block = pl.ds(chunk * CHUNK, CHUNK), feature_block(chunk)
        p_own = lax.dot_general(proj_t[:, :dim], h_normed[rows, :], contract_last, preferred_element_type=F32)
        p_own = p_own + lax.dot_general(proj_t[:, dim:], e_full[rows, :], contract_last, preferred_element_type=F32)
        p_full[block(me)] = p_own.astype(BF16)
        live[chunk] = gather_start(p_full, block, 1, chunk)

    def p_pass(chunk):
        live[chunk] = gather_pass(live[chunk], p_full, feature_block(chunk), 1, chunk)

    def feed_forward(chunk):
        gather_end(live[chunk])
        lanes = pl.ds(chunk * CHUNK, CHUNK)
        norm_columns(p_full.at[:, lanes], n_full.at[:, lanes], gain_row(gains, 2))
        gate_val = jnp.dot(gate_t[...], n_full[:, lanes], preferred_element_type=F32)
        up_val = jnp.dot(up_t[...], n_full[:, lanes], preferred_element_type=F32)
        a_full[:, lanes] = (gate_val * jax.nn.sigmoid(gate_val) * up_val).astype(BF16)
        part_d[:, lanes] = lax.dot_general(down[...], a_full[:, lanes], contract_first, preferred_element_type=F32)
        live[chunk] = pair_send(part_d, feature_block(chunk), pair_d, 2, chunk)

    def d_mid(chunk):
        for copy in live[chunk]:
            copy.wait()
        block, sends = feature_block(chunk), {}
        for k in order + [0]:
            pair_d[chunk, far[k]] = part_d[block(far[k] * 2 + core)] + pair_d[chunk, far[k]]
            if k:
                sends[k] = far_send(pair_d.at[chunk, far[k]], far_d, k, 3, chunk)
        live[chunk] = sends

    def d_end(chunk):
        summed = pair_d[chunk, chip]
        for k in [1, 3, 2]:
            live[chunk][k].wait()
            summed = summed + far_d[chunk, k - 1]
        block = feature_block(chunk)
        u_full[block(me)] = (p_full[block(me)].astype(F32) + summed).astype(BF16)
        live[chunk] = gather_start(u_full, block, 2, chunk)

    def u_pass(chunk):
        live[chunk] = gather_pass(live[chunk], u_full, feature_block(chunk), 2, chunk)

    def finish(chunk):
        gather_end(live[chunk])
        lanes = pl.ds(chunk * CHUNK, CHUNK)
        norm_columns(u_full.at[:, lanes], o_ref.at[:, lanes], gain_row(gains, 3))
        for start in range(chunk * CHUNK, (chunk + 1) * CHUNK, 128):
            u_ref[pl.ds(start, 128), :] = u_full[:, pl.ds(start, 128)].T

    for stage in (e_start, e_mid, h_norm, e_end, e_pass, project, p_pass, feed_forward, d_mid, d_end, u_pass, finish):
        for chunk in range(chunks):
            stage(chunk)


def mix(n_tp, hidden, picked, gains, proj_w, w_gate, w_up, w_down):
    tokens, dim = hidden.shape
    chips, chunks = n_tp // 2, tokens // CHUNK
    t_rows, f_rows, ffn = CHUNK // n_tp, proj_w.shape[1], w_gate.shape[1]
    vmem = pl.BlockSpec(memory_space=pltpu.VMEM)
    return pl.pallas_call(
        functools.partial(mix_kernel, n_tp),
        out_shape=(jax.ShapeDtypeStruct((tokens, dim), BF16), jax.ShapeDtypeStruct((dim, tokens), BF16)),
        in_specs=[vmem] * 7,
        out_specs=(vmem, vmem),
        scratch_shapes=[
            pltpu.VMEM((tokens, dim), BF16),
            pltpu.VMEM((tokens, dim), BF16),
            pltpu.VMEM((dim, tokens), BF16),
            pltpu.VMEM((dim, tokens), BF16),
            pltpu.VMEM((ffn, tokens), BF16),
            pltpu.VMEM((dim, tokens), BF16),
            pltpu.VMEM((chunks, chips, t_rows, dim), BF16),
            pltpu.VMEM((chunks, chips, t_rows, dim), BF16),
            pltpu.VMEM((chunks, chips - 1, t_rows, dim), BF16),
            pltpu.VMEM((dim, tokens), F32),
            pltpu.VMEM((chunks, chips, f_rows, CHUNK), F32),
            pltpu.VMEM((chunks, chips - 1, f_rows, CHUNK), F32),
            pltpu.SemaphoreType.DMA((4, chunks, chips)),
            pltpu.SemaphoreType.DMA((4, chunks, chips)),
            pltpu.SemaphoreType.DMA((3, chunks, 2 * chips)),
            pltpu.SemaphoreType.DMA((3, chunks, 2 * chips)),
        ],
        compiler_params=pltpu.CompilerParams(collective_id=0, has_side_effects=True, vmem_limit_bytes=48 << 20),
        name="mix",
    )(hidden, picked, gains, proj_w.T, w_gate.T, w_up.T, w_down)


def stats_kernel(n_keep, keep_tiles, head_ref, o_ref, *refs):
    keeps, (max_ref, sum_ref, slots, held, base, sems) = refs[:n_keep], refs[n_keep:]
    each = keep_tiles // n_keep
    vocab, tokens = head_ref.shape[0], o_ref.shape[1]
    full, tail = vocab // TILE, vocab % TILE
    depth = slots.shape[0]

    def fetch(tile, rows):
        slot = lax.rem(tile, depth)
        return pltpu.make_async_copy(
            head_ref.at[pl.ds(pl.multiple_of(tile * TILE, 16), rows), :],
            slots.at[slot, pl.ds(0, rows), :],
            sems.at[slot],
        )

    def fetch_any(tile):
        @pl.when(tile < full)
        def _():
            fetch(tile, TILE).start()

        if tail:

            @pl.when(tile == full)
            def _():
                fetch(tile, tail).start()

    def parts(rows):
        return [(top, min(HALF, rows - top)) for top in range(0, rows, HALF)]

    def groups(z):
        return z.reshape(z.shape[0] // 8, 8, z.shape[1])

    def rescale(lanes):
        top = max_ref[:, lanes]
        sum_ref[:, lanes] = sum_ref[:, lanes] * jnp.exp(base[:, lanes] - top)
        base[:, lanes] = top

    def add_held(top, size, lanes):
        z = groups(held[pl.ds(top, size), lanes])
        sum_ref[:, lanes] = sum_ref[:, lanes] + jnp.sum(jnp.exp(z - base[:, lanes][None]), axis=0)

    def work(tile, rows, keep):
        slot = lax.rem(tile, depth)
        for start in range(0, tokens, LANES):
            lanes = pl.ds(start, LANES)
            rescale(lanes)
            for top, size in parts(TILE):
                add_held(top, size, lanes)
                size = min(size, rows - top)
                z = jnp.dot(slots[slot, pl.ds(top, size), :], o_ref[:, lanes], preferred_element_type=F32)
                if keep is not None:
                    keeps[keep][pl.ds(pl.multiple_of((tile - keep * each) * TILE + top, 16), size), lanes] = z
                held[pl.ds(top, size), lanes] = z
                max_ref[:, lanes] = jnp.maximum(max_ref[:, lanes], jnp.max(groups(z), axis=0))

    for tile in range(depth - 1):
        fetch(tile, TILE).start()
    max_ref[...] = jnp.full_like(max_ref, LOWEST)
    base[...] = jnp.full_like(base, LOWEST)
    sum_ref[...] = jnp.zeros_like(sum_ref)
    held[...] = jnp.full_like(held, -jnp.inf)

    def step(keep, tile, carry):
        fetch_any(tile + depth - 1)
        fetch(tile, TILE).wait()
        work(tile, TILE, keep)
        return carry

    for index in range(n_keep):
        lax.fori_loop(index * each, (index + 1) * each, functools.partial(step, index), 0)
    lax.fori_loop(keep_tiles, full, functools.partial(step, None), 0)
    if tail:
        fetch(full, tail).wait()
        work(full, tail, None)
    for start in range(0, tokens, LANES):
        rescale(pl.ds(start, LANES))
        for top, size in parts(tail or TILE):
            add_held(top, size, pl.ds(start, LANES))


def head_stats(n_keep, keep_tiles, depth, head_t, o_t):
    vocab, dim = head_t.shape
    tokens = o_t.shape[1]
    vmem = pl.BlockSpec(memory_space=pltpu.VMEM)
    return pl.pallas_call(
        functools.partial(stats_kernel, n_keep, keep_tiles),
        out_shape=(*[pltpu.VMEM((keep_tiles // n_keep * TILE, tokens), F32)] * n_keep, jax.ShapeDtypeStruct((8, tokens), F32), jax.ShapeDtypeStruct((8, tokens), F32)),
        in_specs=[pl.BlockSpec(memory_space=pl.ANY), vmem],
        out_specs=(vmem,) * (n_keep + 2),
        scratch_shapes=[pltpu.VMEM((depth, TILE, dim), BF16), pltpu.VMEM((TILE, tokens), F32), pltpu.VMEM((8, tokens), F32), pltpu.SemaphoreType.DMA((depth,))],
        compiler_params=pltpu.CompilerParams(vmem_limit_bytes=12 << 20),
        name="head_stats",
    )(pltpu.with_memory_space_constraint(head_t, pltpu.HBM), o_t)

def merge_kernel(n_tp, max_ref, sum_ref, lse_ref, mine, theirs, send_sem, recv_sem):
    me = lax.axis_index("tp")
    barrier = pltpu.get_barrier_semaphore()
    for k in range(1, n_tp):
        peer = lax.rem(me + k, n_tp)
        pl.semaphore_signal(barrier, inc=1, device_id={"tp": peer}, device_id_type=MESH)
    tokens = max_ref.shape[1]
    top = jnp.max(max_ref[...], axis=0, keepdims=True)
    scaled = jnp.sum(sum_ref[...] * jnp.exp(max_ref[...] - top), axis=0, keepdims=True)
    mine[...] = jnp.concatenate([top, scaled], axis=0)
    pl.semaphore_wait(barrier, n_tp - 1)
    copies = []
    for k in range(1, n_tp):
        copy = pltpu.make_async_remote_copy(
            src_ref=mine,
            dst_ref=theirs.at[k - 1],
            send_sem=send_sem.at[k - 1],
            recv_sem=recv_sem.at[k - 1],
            device_id={"tp": lax.rem(me + k, n_tp)},
            device_id_type=MESH,
        )
        copy.start()
        copies.append(copy)
    for copy in copies:
        copy.wait()
    best, total = top, scaled
    for k in range(n_tp - 1):
        arrived = theirs[k]
        other, extra = arrived[0:1, :], arrived[1:2, :]
        new = jnp.maximum(best, other)
        total = total * jnp.exp(best - new) + extra * jnp.exp(other - new)
        best = new
    lse_ref[...] = jnp.broadcast_to(best + jnp.log(total), lse_ref.shape)


def merge(n_tp, maxima, sums):
    tokens = maxima.shape[1]
    vmem = pl.BlockSpec(memory_space=pltpu.VMEM)
    return pl.pallas_call(
        functools.partial(merge_kernel, n_tp),
        out_shape=jax.ShapeDtypeStruct((8, tokens), F32),
        in_specs=[vmem, vmem],
        out_specs=vmem,
        scratch_shapes=[
            pltpu.VMEM((2, tokens), F32),
            pltpu.VMEM((n_tp - 1, 2, tokens), F32),
            pltpu.SemaphoreType.DMA((n_tp - 1,)),
            pltpu.SemaphoreType.DMA((n_tp - 1,)),
        ],
        compiler_params=pltpu.CompilerParams(collective_id=1, has_side_effects=True, vmem_limit_bytes=2 << 20),
        name="merge",
    )(maxima, sums)


def logp_kernel(n_keep, keep_tiles, head_ref, o_ref, lse_ref, *refs):
    keeps = refs[:n_keep]
    out_ref, slots, made, kept, in_sems, made_sems, kept_sems = refs[n_keep:]
    vocab, tokens = head_ref.shape[0], o_ref.shape[1]
    each = keep_tiles // n_keep * 2
    kept_chunks = keep_tiles * 2
    base = keep_tiles * TILE
    rest = vocab - base
    steps, tail = rest // HALF, rest % HALF
    n_slots = kept.shape[0]
    spans = [steps * (i + 1) // n_keep for i in range(n_keep)]

    def fetch(step, rows):
        slot = lax.rem(step, 2)
        return pltpu.make_async_copy(
            head_ref.at[pl.ds(pl.multiple_of(base + step * HALF, 16), rows), :], slots.at[slot, pl.ds(0, rows), :], in_sems.at[slot])

    def put_made(step, rows):
        slot = lax.rem(step, 2)
        return pltpu.make_async_copy(
            made.at[slot, pl.ds(0, rows), :], out_ref.at[pl.ds(pl.multiple_of(base + step * HALF, 16), rows), :], made_sems.at[slot])

    def put_kept(chunk):
        slot = lax.rem(chunk, n_slots)
        return pltpu.make_async_copy(
            kept.at[slot], out_ref.at[pl.ds(pl.multiple_of(chunk * HALF, 16), HALF), :], kept_sems.at[slot])

    def do_kept(index, chunk):
        @pl.when(chunk >= n_slots)
        def _():
            put_kept(chunk - n_slots).wait()
        slot = lax.rem(chunk, n_slots)
        rows = pl.ds(pl.multiple_of((chunk - index * each) * HALF, 16), HALF)
        for start in range(0, tokens, LANES):
            lanes = pl.ds(start, LANES)
            kept[slot, :, lanes] = keeps[index][rows, lanes] - lse_ref[:, lanes][0:1, :]
        put_kept(chunk).start()

    def make(step, rows):
        slot = lax.rem(step, 2)
        for start in range(0, tokens, LANES):
            lanes = pl.ds(start, LANES)
            z = jnp.dot(slots[slot, pl.ds(0, rows), :], o_ref[:, lanes], preferred_element_type=F32)
            made[slot, pl.ds(0, rows), lanes] = z - lse_ref[:, lanes][0:1, :]

    def start_fetch(step):
        @pl.when(step < steps)
        def _():
            fetch(step, HALF).start()
        if tail:
            @pl.when(step == steps)
            def _():
                fetch(step, tail).start()

    start_fetch(0)
    done_steps = 0
    for index in range(n_keep):
        stop = spans[index]
        count = stop - done_steps
        per_step = each // count if count else 0

        def step_fn(step, carry, index=index, first=done_steps, per_step=per_step):
            start_fetch(step + 1)
            for i in range(per_step):
                do_kept(index, index * each + (step - first) * per_step + i)
            fetch(step, HALF).wait()
            @pl.when(step >= 2)
            def _():
                put_made(step - 2, HALF).wait()
            make(step, HALF)
            put_made(step, HALF).start()
            return carry

        lax.fori_loop(done_steps, stop, step_fn, 0)

        def kept_fn(chunk, carry, index=index):
            do_kept(index, chunk)
            return carry
        lax.fori_loop(index * each + count * per_step, (index + 1) * each, kept_fn, 0)
        done_steps = stop
    if tail:
        fetch(steps, tail).wait()
        put_made(steps - 2, HALF).wait()
        make(steps, tail)
        put_made(steps, tail).start()
        put_made(steps - 1, HALF).wait()
        put_made(steps, tail).wait()
    else:
        put_made(steps - 2, HALF).wait()
        put_made(steps - 1, HALF).wait()
    for i in range(n_slots):
        put_kept(kept_chunks - n_slots + i).wait()

def head_logp(n_keep, keep_tiles, n_kept, head_t, o_t, keeps, lse):
    vocab, dim = head_t.shape
    tokens = o_t.shape[1]
    vmem = pl.BlockSpec(memory_space=pltpu.VMEM)
    anym = pl.BlockSpec(memory_space=pl.ANY)
    return pl.pallas_call(
        functools.partial(logp_kernel, n_keep, keep_tiles),
        out_shape=jax.ShapeDtypeStruct((vocab, tokens), F32),
        in_specs=[anym] + [vmem] * (n_keep + 2),
        out_specs=anym,
        scratch_shapes=[
            pltpu.VMEM((2, HALF, dim), BF16),
            pltpu.VMEM((2, HALF, tokens), F32),
            pltpu.VMEM((n_kept, HALF, tokens), F32),
            pltpu.SemaphoreType.DMA((2,)), pltpu.SemaphoreType.DMA((2,)), pltpu.SemaphoreType.DMA((n_kept,)),
        ],
        compiler_params=pltpu.CompilerParams(vmem_limit_bytes=14 << 20),
        name="head_logp",
    )(pltpu.with_memory_space_constraint(head_t, pltpu.HBM), o_t, lse, *[pltpu.with_memory_space_constraint(keep, pltpu.VMEM) for keep in keeps])


def solution(mesh):
    n_tp = mesh.shape["tp"]

    def draft_step(hidden, tokens, embedding, head_w, h_norm, e_norm, f_norm, o_norm, proj_w, w_gate, w_up, w_down):
        vocab_local = embedding.shape[0]
        local_ids = tokens - lax.axis_index("tp") * vocab_local
        owned = (local_ids >= 0) & (local_ids < vocab_local)
        picked = gather_rows(embedding, local_ids, owned)
        gains = jnp.concatenate([h_norm, e_norm, f_norm, o_norm]).reshape(-1, 128)
        new_u, out_t = mix(n_tp, hidden, picked, gains, proj_w, w_gate, w_up, w_down)
        head_t = head_w.T
        *keeps, maxima, sums = head_stats(KEEPS, KEEP_TILES, 3, head_t, out_t)
        lse = merge(n_tp, maxima, sums)
        return new_u, head_logp(KEEPS, KEEP_TILES, 3, head_t, out_t, keeps, lse).T

    specs_in = (
        P("dp", None), P("dp"), P("tp", None), P(None, "tp"), P(None), P(None), P(None), P(None),
        P(None, "tp"), P(None, "tp"), P(None, "tp"), P("tp", None),
    )
    specs_out = (P("dp", None), P("dp", "tp"))
    return jax.shard_map(draft_step, mesh=mesh, in_specs=specs_in, out_specs=specs_out, check_vma=False)
```

```python
import functools

import jax
import jax.numpy as jnp
from jax import lax
from jax.experimental import pallas as pl
from jax.experimental.pallas import tpu as pltpu
from jax.sharding import PartitionSpec as P

NORM_EPS = 1e-6
SLAB = 8
GROUP = 32
TILE = 1056
HALF = TILE // 2
LANES = 256
KEEPS = 6
KEEP_TILES = 12
CHUNK = 256
LAG = 0
LOWEST = float(jnp.finfo(jnp.float32).min)
F32 = jnp.float32
BF16 = jnp.bfloat16
MESH = pl.DeviceIdType.MESH


def gather_kernel(base_ref, want_ref, table_ref, out_ref, slabs, sems):
    groups = out_ref.shape[0] // GROUP
    span = GROUP * SLAB

    def issue(group, carry):
        for lane in range(GROUP):
            row = group * GROUP + lane
            base = pl.multiple_of(base_ref[row], SLAB)
            pltpu.make_async_copy(
                table_ref.at[pl.ds(base, SLAB), :],
                slabs.at[pl.ds(pl.multiple_of(row * SLAB, SLAB), SLAB), :],
                sems.at[group],
            ).start()
        return carry

    lax.fori_loop(0, groups, issue, 0)

    def select(group, carry):
        block = pl.ds(pl.multiple_of(group * span, span), span)
        rows = pl.ds(pl.multiple_of(group * GROUP, GROUP), GROUP)
        pltpu.make_async_copy(table_ref.at[pl.ds(0, span), :], slabs.at[block, :], sems.at[group]).wait()
        lanes = lax.broadcasted_iota(jnp.int32, (GROUP, span), 1)
        hot = jnp.where(want_ref[rows, :] == lanes, 1.0, 0.0).astype(BF16)
        out_ref[rows, :] = jnp.dot(hot, slabs[block, :], preferred_element_type=F32).astype(BF16)
        return carry

    lax.fori_loop(0, groups, select, 0)


def gather_rows(embedding, local_ids, owned):
    rows, dim = local_ids.shape[0], embedding.shape[1]
    spread = jnp.arange(rows, dtype=jnp.int32)
    ids = jnp.where(owned, local_ids, spread * SLAB % embedding.shape[0])
    place = spread % GROUP
    want = jnp.where(owned, place * SLAB + ids % SLAB, -1)[:, None]
    return pl.pallas_call(
        gather_kernel,
        out_shape=pltpu.VMEM((rows, dim), BF16),
        in_specs=[
            pl.BlockSpec(memory_space=pltpu.SMEM),
            pl.BlockSpec(memory_space=pltpu.VMEM),
            pl.BlockSpec(memory_space=pl.ANY),
        ],
        out_specs=pl.BlockSpec(memory_space=pltpu.VMEM),
        scratch_shapes=[
            pltpu.VMEM((rows * SLAB, dim), BF16),
            pltpu.SemaphoreType.DMA((rows // GROUP,)),
        ],
        compiler_params=pltpu.CompilerParams(vmem_limit_bytes=24 << 20),
        name="gather_rows",
    )(ids // SLAB * SLAB, want, embedding)


def gain_row(gains, index):
    packed = gains[...]
    count = packed.shape[0] // 4
    return jnp.concatenate([packed[index * count + j : index * count + j + 1, :] for j in range(count)], axis=1)


def column_of(gain):
    return jnp.broadcast_to(gain, (128, gain.shape[1])).T


def norm_columns(src_ref, dst_ref, gain_ref):
    gain = gain_ref[...]
    dim, tokens = src_ref.shape
    for start in range(0, tokens, 128):
        lanes = pl.ds(start, 128)
        wide = src_ref[:, lanes].astype(F32)
        inv_rms = lax.rsqrt(jnp.sum(wide * wide, axis=0, keepdims=True) / dim + NORM_EPS)
        dst_ref[:, lanes] = (wide * inv_rms * gain).astype(dst_ref.dtype)


def norm_rows(wide, gain):
    inv_rms = lax.rsqrt(jnp.mean(wide * wide, axis=-1, keepdims=True) + NORM_EPS)
    return (wide * inv_rms * gain).astype(BF16)


def mix_kernel(
    n_tp,
    hidden_ref,
    picked_ref,
    gains,
    proj_t,
    gate_t,
    up_t,
    down,
    u_ref,
    o_ref,
    columns,
    down_t,
    h_normed,
    e_full,
    p_full,
    n_full,
    a_full,
    u_full,
    comb_e,
    pair_e,
    half_e,
    far_e,
    part_d,
    pair_d,
    comb_d,
    half_d,
    far_d,
    send_rs,
    recv_rs,
    send_ag,
    recv_ag,
):
    me = lax.axis_index("tp")
    chips = n_tp // 2
    chip, core = me // 2, me % 2
    partner = chip * 2 + 1 - core
    far = [lax.rem(chip + k, chips) for k in range(chips)]
    back = [lax.rem(chip + chips - k, chips) for k in range(chips)]
    tokens, dim = hidden_ref.shape
    chunks = tokens // CHUNK
    t_rows = CHUNK // n_tp
    f_rows = proj_t.shape[0]
    contract_last = (((1,), (1,)), ((), ()))

    barrier = pltpu.get_barrier_semaphore()
    for peer in [partner] + [far[k] * 2 + core for k in range(1, chips)]:
        pl.semaphore_signal(barrier, inc=1, device_id={"tp": peer}, device_id_type=MESH)
    for start in range(0, tokens, 64):
        rows = pl.ds(start, 64)
        h_normed[rows, :] = norm_rows(hidden_ref[rows, :].astype(F32), gain_row(gains, 0))
    columns[0] = column_of(gain_row(gains, 2))
    columns[1] = column_of(gain_row(gains, 3))
    down_t[...] = down[...].T
    pl.semaphore_wait(barrier, chips)

    def push(src, dst, send_sem, recv_sem, device):
        copy = pltpu.make_async_remote_copy(
            src_ref=src, dst_ref=dst, send_sem=send_sem, recv_sem=recv_sem, device_id={"tp": device}, device_id_type=MESH
        )
        copy.start()
        return copy

    def token_block(chunk):
        return lambda device: (pl.ds(pl.multiple_of(chunk * CHUNK + device * t_rows, 16), t_rows), slice(None))

    def feature_block(chunk):
        return lambda device: (pl.ds(pl.multiple_of(device * f_rows, 16), f_rows), pl.ds(chunk * CHUNK, CHUNK))

    def pair_send(src, block, landing, stage, chunk):
        return [
            push(
                src.at[block(c * 2 + 1 - core)],
                landing.at[chunk, c],
                send_rs.at[stage, chunk, c],
                recv_rs.at[stage, chunk, c],
                partner,
            )
            for c in range(chips)
        ]

    def halves(block):
        rows, lanes = block
        if isinstance(lanes, slice):
            half = t_rows // 2
            return [(pl.ds(pl.multiple_of(rows.start + half * side, 16), half), lanes) for side in range(2)]
        half = CHUNK // 2
        return [(rows, pl.ds(lanes.start + half * side, half)) for side in range(2)]

    def neighbour_halves(shape):
        if shape[0] == t_rows:
            return [(pl.ds(t_rows // 2 * side, t_rows // 2), slice(None)) for side in range(2)]
        return [(slice(None), pl.ds(CHUNK // 2 * side, CHUNK // 2)) for side in range(2)]

    def across_send(sums, landing, stage, chunk):
        parts = neighbour_halves(sums.shape[2:])
        return [
            push(
                sums.at[(chunk, 2) + parts[side]],
                landing.at[chunk, side],
                send_rs.at[stage, chunk, side],
                recv_rs.at[stage, chunk, side],
                far[k] * 2 + core,
            )
            for side, k in ((0, 1), (1, 3))
        ]

    def next_send(sums, across, landing, into, stage, chunk):
        parts = neighbour_halves(sums.shape[2:])
        sends = []
        for side, k in ((0, 1), (1, 3)):
            across[side].wait()
            view = (chunk, k) + parts[side]
            sums[view] = sums[view] + landing[chunk, side]
            sends.append(
                push(
                    sums.at[chunk, k],
                    into.at[chunk, side],
                    send_rs.at[stage, chunk, side],
                    recv_rs.at[stage, chunk, side],
                    far[k] * 2 + core,
                )
            )
        return sends

    def gather_start(full, block, stage, chunk):
        own = full.at[block(me)]
        sends = {
            k: push(own, own, send_ag.at[stage, chunk, k], recv_ag.at[stage, chunk, k], far[k] * 2 + core) for k in (2, 1, 3)
        }
        near = push(own, own, send_ag.at[stage, chunk, 0], recv_ag.at[stage, chunk, 0], partner)
        return sends, near

    def gather_pass(state, full, block, stage, chunk):
        sends, near = state
        passed = []
        for k in [1, 3, 2]:
            sends[k].wait_recv()
            view = full.at[block(back[k] * 2 + core)]
            passed.append(
                push(view, view, send_ag.at[stage, chunk, chips + k], recv_ag.at[stage, chunk, chips + k], partner)
            )
        return [near] + passed, list(sends.values())

    def gather_end(state):
        local, sends = state
        for copy in local:
            copy.wait()
        for copy in sends:
            copy.wait_send()

    live = [None] * chunks

    def e_start(chunk):
        live[chunk] = pair_send(picked_ref, token_block(chunk), pair_e, 0, chunk)

    def e_mid(chunk):
        for copy in live[chunk]:
            copy.wait()
        block, across = token_block(chunk), None
        for k in (2, 1, 3, 0):
            comb_e[chunk, k] = picked_ref[block(far[k] * 2 + core)] + pair_e[chunk, far[k]]
            across = across_send(comb_e, half_e, 1, chunk) if k == 2 else across
        live[chunk] = across

    def e_next(chunk):
        live[chunk] = next_send(comb_e, live[chunk], half_e, far_e, 4, chunk)

    def e_end(chunk):
        total = comb_e[chunk, 0]
        for side in range(2):
            live[chunk][side].wait()
            total = total + far_e[chunk, side]
        block = token_block(chunk)
        e_full[block(me)] = norm_rows(total.astype(F32), gain_row(gains, 1))
        live[chunk] = gather_start(e_full, block, 0, chunk)

    def e_pass(chunk):
        live[chunk] = gather_pass(live[chunk], e_full, token_block(chunk), 0, chunk)

    def project(chunk):
        gather_end(live[chunk])
        rows, block = pl.ds(chunk * CHUNK, CHUNK), feature_block(chunk)
        p_own = lax.dot_general(proj_t[:, :dim], h_normed[rows, :], contract_last, preferred_element_type=F32)
        p_own = p_own + lax.dot_general(proj_t[:, dim:], e_full[rows, :], contract_last, preferred_element_type=F32)
        p_full[block(me)] = p_own.astype(BF16)
        live[chunk] = gather_start(p_full, block, 1, chunk)

    def p_pass(chunk):
        live[chunk] = gather_pass(live[chunk], p_full, feature_block(chunk), 1, chunk)

    def feed_forward(chunk):
        gather_end(live[chunk])
        lanes = pl.ds(chunk * CHUNK, CHUNK)
        norm_columns(p_full.at[:, lanes], n_full.at[:, lanes], columns.at[0])
        gate_val = jnp.dot(gate_t[...], n_full[:, lanes], preferred_element_type=F32)
        up_val = jnp.dot(up_t[...], n_full[:, lanes], preferred_element_type=F32)
        a_full[:, lanes] = (gate_val * jax.nn.sigmoid(gate_val) * up_val).astype(BF16)
        part_d[:, lanes] = jnp.dot(down_t[...], a_full[:, lanes], preferred_element_type=F32)
        live[chunk] = pair_send(part_d, feature_block(chunk), pair_d, 2, chunk)

    def d_mid(chunk):
        for copy in live[chunk]:
            copy.wait()
        block, across = feature_block(chunk), None
        for k in (2, 1, 3, 0):
            comb_d[chunk, k] = part_d[block(far[k] * 2 + core)] + pair_d[chunk, far[k]]
            across = across_send(comb_d, half_d, 3, chunk) if k == 2 else across
        live[chunk] = across

    def d_next(chunk):
        live[chunk] = next_send(comb_d, live[chunk], half_d, far_d, 5, chunk)

    def d_end(chunk):
        summed = comb_d[chunk, 0]
        for side in range(2):
            live[chunk][side].wait()
            summed = summed + far_d[chunk, side]
        block = feature_block(chunk)
        u_full[block(me)] = (p_full[block(me)].astype(F32) + summed).astype(BF16)
        live[chunk] = gather_start(u_full, block, 2, chunk)

    def u_pass(chunk):
        live[chunk] = gather_pass(live[chunk], u_full, feature_block(chunk), 2, chunk)

    def finish(chunk):
        gather_end(live[chunk])
        lanes = pl.ds(chunk * CHUNK, CHUNK)
        norm_columns(u_full.at[:, lanes], o_ref.at[:, lanes], columns.at[1])
        for start in range(chunk * CHUNK, (chunk + 1) * CHUNK, 128):
            u_ref[pl.ds(start, 128), :] = u_full[:, pl.ds(start, 128)].T

    stages = (
        e_start, e_mid, e_next, e_end, e_pass, project, p_pass, feed_forward,
        d_mid, d_next, d_end, u_pass, finish,
    )
    turns = sorted((index + LAG * chunk, chunk, index) for index in range(len(stages)) for chunk in range(chunks))
    for _, chunk, index in turns:
        stages[index](chunk)


def mix(n_tp, hidden, picked, gains, proj_w, w_gate, w_up, w_down):
    tokens, dim = hidden.shape
    chips, chunks = n_tp // 2, tokens // CHUNK
    t_rows, f_rows, ffn = CHUNK // n_tp, proj_w.shape[1], w_gate.shape[1]
    vmem = pl.BlockSpec(memory_space=pltpu.VMEM)
    return pl.pallas_call(
        functools.partial(mix_kernel, n_tp),
        out_shape=(jax.ShapeDtypeStruct((tokens, dim), BF16), pltpu.VMEM((dim, tokens), BF16)),
        in_specs=[vmem] * 7,
        out_specs=(vmem, vmem),
        scratch_shapes=[
            pltpu.VMEM((2, dim, 128), F32),
            pltpu.VMEM((dim, ffn), BF16),
            pltpu.VMEM((tokens, dim), BF16),
            pltpu.VMEM((tokens, dim), BF16),
            pltpu.VMEM((dim, tokens), BF16),
            pltpu.VMEM((dim, tokens), BF16),
            pltpu.VMEM((ffn, tokens), BF16),
            pltpu.VMEM((dim, tokens), BF16),
            pltpu.VMEM((chunks, chips, t_rows, dim), BF16),
            pltpu.VMEM((chunks, chips, t_rows, dim), BF16),
            pltpu.VMEM((chunks, 2, t_rows // 2, dim), BF16),
            pltpu.VMEM((chunks, 2, t_rows, dim), BF16),
            pltpu.VMEM((dim, tokens), F32),
            pltpu.VMEM((chunks, chips, f_rows, CHUNK), F32),
            pltpu.VMEM((chunks, chips, f_rows, CHUNK), F32),
            pltpu.VMEM((chunks, 2, f_rows, CHUNK // 2), F32),
            pltpu.VMEM((chunks, 2, f_rows, CHUNK), F32),
            pltpu.SemaphoreType.DMA((6, chunks, chips)),
            pltpu.SemaphoreType.DMA((6, chunks, chips)),
            pltpu.SemaphoreType.DMA((3, chunks, 10)),
            pltpu.SemaphoreType.DMA((3, chunks, 10)),
        ],
        compiler_params=pltpu.CompilerParams(collective_id=0, has_side_effects=True, vmem_limit_bytes=32 << 20),
        name="mix",
    )(*[pltpu.with_memory_space_constraint(x, pltpu.VMEM) for x in (hidden, picked, gains, proj_w.T, w_gate.T, w_up.T, w_down)])


def stats_kernel(n_tp, n_keep, keep_tiles, head_ref, o_ref, lse_ref, *refs):
    keeps = refs[:n_keep]
    max_ref, sum_ref, slots, held, base, mine, theirs, sems, send_sem, recv_sem = refs[n_keep:]
    me = lax.axis_index("tp")
    peers = [lax.rem(me + k, n_tp) for k in range(1, n_tp)]
    barrier = pltpu.get_barrier_semaphore()
    for peer in peers:
        pl.semaphore_signal(barrier, inc=1, device_id={"tp": peer}, device_id_type=MESH)
    each = keep_tiles // n_keep
    vocab, tokens = head_ref.shape[0], o_ref.shape[1]
    full, tail = vocab // TILE, vocab % TILE
    depth = slots.shape[0]

    def fetch(tile, rows):
        slot = lax.rem(tile, depth)
        return pltpu.make_async_copy(
            head_ref.at[pl.ds(pl.multiple_of(tile * TILE, 16), rows), :],
            slots.at[slot, pl.ds(0, rows), :],
            sems.at[slot],
        )

    def fetch_any(tile):
        @pl.when(tile < full)
        def _():
            fetch(tile, TILE).start()

        if tail:

            @pl.when(tile == full)
            def _():
                fetch(tile, tail).start()

    def parts(rows):
        return [(top, min(HALF, rows - top)) for top in range(0, rows, HALF)]

    def groups(z):
        return z.reshape(z.shape[0] // 8, 8, z.shape[1])

    def rescale(lanes):
        top = max_ref[:, lanes]
        sum_ref[:, lanes] = sum_ref[:, lanes] * jnp.exp(base[:, lanes] - top)
        base[:, lanes] = top

    def add_held(top, size, lanes):
        z = groups(held[pl.ds(top, size), lanes])
        sum_ref[:, lanes] = sum_ref[:, lanes] + jnp.sum(jnp.exp(z - base[:, lanes][None]), axis=0)

    def work(tile, rows, keep):
        slot = lax.rem(tile, depth)
        for start in range(0, tokens, LANES):
            lanes = pl.ds(start, LANES)
            rescale(lanes)
            for top, size in parts(TILE):
                add_held(top, size, lanes)
                size = min(size, rows - top)
                z = jnp.dot(slots[slot, pl.ds(top, size), :], o_ref[:, lanes], preferred_element_type=F32)
                if keep is not None:
                    keeps[keep][pl.ds(pl.multiple_of((tile - keep * each) * TILE + top, 16), size), lanes] = z
                held[pl.ds(top, size), lanes] = z
                max_ref[:, lanes] = jnp.maximum(max_ref[:, lanes], jnp.max(groups(z), axis=0))

    for tile in range(depth - 1):
        fetch(tile, TILE).start()
    max_ref[...] = jnp.full_like(max_ref, LOWEST)
    base[...] = jnp.full_like(base, LOWEST)
    sum_ref[...] = jnp.zeros_like(sum_ref)
    held[...] = jnp.full_like(held, -jnp.inf)

    def step(keep, tile, carry):
        fetch_any(tile + depth - 1)
        fetch(tile, TILE).wait()
        work(tile, TILE, keep)
        return carry

    for index in range(n_keep):
        lax.fori_loop(index * each, (index + 1) * each, functools.partial(step, index), 0)
    lax.fori_loop(keep_tiles, full, functools.partial(step, None), 0)
    if tail:
        fetch(full, tail).wait()
        work(full, tail, None)
    for start in range(0, tokens, LANES):
        rescale(pl.ds(start, LANES))
        for top, size in parts(tail or TILE):
            add_held(top, size, pl.ds(start, LANES))

    best = jnp.max(max_ref[...], axis=0, keepdims=True)
    total = jnp.sum(sum_ref[...] * jnp.exp(max_ref[...] - best), axis=0, keepdims=True)
    mine[...] = jnp.concatenate([best, total], axis=0)
    pl.semaphore_wait(barrier, n_tp - 1)
    copies = []
    for k, peer in enumerate(peers):
        copy = pltpu.make_async_remote_copy(
            src_ref=mine,
            dst_ref=theirs.at[k],
            send_sem=send_sem.at[k],
            recv_sem=recv_sem.at[k],
            device_id={"tp": peer},
            device_id_type=MESH,
        )
        copy.start()
        copies.append(copy)
    for k, copy in enumerate(copies):
        copy.wait()
        arrived = theirs[k]
        other, extra = arrived[0:1, :], arrived[1:2, :]
        new = jnp.maximum(best, other)
        total = total * jnp.exp(best - new) + extra * jnp.exp(other - new)
        best = new
    lse_ref[...] = jnp.broadcast_to(best + jnp.log(total), lse_ref.shape)


def head_stats(n_tp, n_keep, keep_tiles, depth, head_t, o_t):
    vocab, dim = head_t.shape
    tokens = o_t.shape[1]
    vmem = pl.BlockSpec(memory_space=pltpu.VMEM)
    return pl.pallas_call(
        functools.partial(stats_kernel, n_tp, n_keep, keep_tiles),
        out_shape=(
            jax.ShapeDtypeStruct((8, tokens), F32),
            *[pltpu.VMEM((keep_tiles // n_keep * TILE, tokens), F32)] * n_keep,
        ),
        in_specs=[pl.BlockSpec(memory_space=pl.ANY), vmem],
        out_specs=(vmem,) * (n_keep + 1),
        scratch_shapes=[
            pltpu.VMEM((8, tokens), F32),
            pltpu.VMEM((8, tokens), F32),
            pltpu.VMEM((depth, TILE, dim), BF16),
            pltpu.VMEM((TILE, tokens), F32),
            pltpu.VMEM((8, tokens), F32),
            pltpu.VMEM((2, tokens), F32),
            pltpu.VMEM((n_tp - 1, 2, tokens), F32),
            pltpu.SemaphoreType.DMA((depth,)),
            pltpu.SemaphoreType.DMA((n_tp - 1,)),
            pltpu.SemaphoreType.DMA((n_tp - 1,)),
        ],
        compiler_params=pltpu.CompilerParams(collective_id=1, has_side_effects=True, vmem_limit_bytes=12 << 20),
        name="head_stats",
    )(pltpu.with_memory_space_constraint(head_t, pltpu.HBM), pltpu.with_memory_space_constraint(o_t, pltpu.VMEM))


def logp_kernel(n_keep, keep_tiles, head_ref, o_ref, lse_ref, *refs):
    keeps = refs[:n_keep]
    out_ref, slots, made, kept, in_sems, made_sems, kept_sems = refs[n_keep:]
    vocab, tokens = head_ref.shape[0], o_ref.shape[1]
    each = keep_tiles // n_keep * 2
    kept_chunks = keep_tiles * 2
    base = keep_tiles * TILE
    rest = vocab - base
    steps, tail = rest // HALF, rest % HALF
    n_slots = kept.shape[0]
    spans = [steps * (i + 1) // n_keep for i in range(n_keep)]

    def fetch(step, rows):
        slot = lax.rem(step, 2)
        return pltpu.make_async_copy(
            head_ref.at[pl.ds(pl.multiple_of(base + step * HALF, 16), rows), :], slots.at[slot, pl.ds(0, rows), :], in_sems.at[slot])

    def put_made(step, rows):
        slot = lax.rem(step, 2)
        return pltpu.make_async_copy(
            made.at[slot, pl.ds(0, rows), :], out_ref.at[pl.ds(pl.multiple_of(base + step * HALF, 16), rows), :], made_sems.at[slot])

    def put_kept(chunk):
        slot = lax.rem(chunk, n_slots)
        return pltpu.make_async_copy(
            kept.at[slot], out_ref.at[pl.ds(pl.multiple_of(chunk * HALF, 16), HALF), :], kept_sems.at[slot])

    def do_kept(index, chunk):
        @pl.when(chunk >= n_slots)
        def _():
            put_kept(chunk - n_slots).wait()
        slot = lax.rem(chunk, n_slots)
        rows = pl.ds(pl.multiple_of((chunk - index * each) * HALF, 16), HALF)
        for start in range(0, tokens, LANES):
            lanes = pl.ds(start, LANES)
            kept[slot, :, lanes] = keeps[index][rows, lanes] - lse_ref[:, lanes][0:1, :]
        put_kept(chunk).start()

    def make(step, rows):
        slot = lax.rem(step, 2)
        for start in range(0, tokens, LANES):
            lanes = pl.ds(start, LANES)
            z = jnp.dot(slots[slot, pl.ds(0, rows), :], o_ref[:, lanes], preferred_element_type=F32)
            made[slot, pl.ds(0, rows), lanes] = z - lse_ref[:, lanes][0:1, :]

    def start_fetch(step):
        @pl.when(step < steps)
        def _():
            fetch(step, HALF).start()
        if tail:
            @pl.when(step == steps)
            def _():
                fetch(step, tail).start()

    start_fetch(0)
    done_steps = 0
    for index in range(n_keep):
        stop = spans[index]
        count = stop - done_steps
        per_step = each // count if count else 0

        def step_fn(step, carry, index=index, first=done_steps, per_step=per_step):
            start_fetch(step + 1)
            for i in range(per_step):
                do_kept(index, index * each + (step - first) * per_step + i)
            fetch(step, HALF).wait()
            @pl.when(step >= 2)
            def _():
                put_made(step - 2, HALF).wait()
            make(step, HALF)
            put_made(step, HALF).start()
            return carry

        lax.fori_loop(done_steps, stop, step_fn, 0)

        def kept_fn(chunk, carry, index=index):
            do_kept(index, chunk)
            return carry
        lax.fori_loop(index * each + count * per_step, (index + 1) * each, kept_fn, 0)
        done_steps = stop
    if tail:
        fetch(steps, tail).wait()
        put_made(steps - 2, HALF).wait()
        make(steps, tail)
        put_made(steps, tail).start()
        put_made(steps - 1, HALF).wait()
        put_made(steps, tail).wait()
    else:
        put_made(steps - 2, HALF).wait()
        put_made(steps - 1, HALF).wait()
    for i in range(n_slots):
        put_kept(kept_chunks - n_slots + i).wait()

def head_logp(n_keep, keep_tiles, n_kept, head_t, o_t, keeps, lse):
    vocab, dim = head_t.shape
    tokens = o_t.shape[1]
    vmem = pl.BlockSpec(memory_space=pltpu.VMEM)
    anym = pl.BlockSpec(memory_space=pl.ANY)
    return pl.pallas_call(
        functools.partial(logp_kernel, n_keep, keep_tiles),
        out_shape=jax.ShapeDtypeStruct((vocab, tokens), F32),
        in_specs=[anym] + [vmem] * (n_keep + 2),
        out_specs=anym,
        scratch_shapes=[
            pltpu.VMEM((2, HALF, dim), BF16),
            pltpu.VMEM((2, HALF, tokens), F32),
            pltpu.VMEM((n_kept, HALF, tokens), F32),
            pltpu.SemaphoreType.DMA((2,)), pltpu.SemaphoreType.DMA((2,)), pltpu.SemaphoreType.DMA((n_kept,)),
        ],
        compiler_params=pltpu.CompilerParams(vmem_limit_bytes=14 << 20),
        name="head_logp",
    )(pltpu.with_memory_space_constraint(head_t, pltpu.HBM), pltpu.with_memory_space_constraint(o_t, pltpu.VMEM), lse, *[pltpu.with_memory_space_constraint(keep, pltpu.VMEM) for keep in keeps])


def solution(mesh):
    n_tp = mesh.shape["tp"]

    def draft_step(hidden, tokens, embedding, head_w, h_norm, e_norm, f_norm, o_norm, proj_w, w_gate, w_up, w_down):
        vocab_local = embedding.shape[0]
        local_ids = tokens - lax.axis_index("tp") * vocab_local
        owned = (local_ids >= 0) & (local_ids < vocab_local)
        picked = gather_rows(embedding, local_ids, owned)
        gains = jnp.concatenate([h_norm, e_norm, f_norm, o_norm]).reshape(-1, 128)
        new_u, out_t = mix(n_tp, hidden, picked, gains, proj_w, w_gate, w_up, w_down)
        head_t = head_w.T
        lse, *keeps = head_stats(n_tp, KEEPS, KEEP_TILES, 3, head_t, out_t)
        return new_u, head_logp(KEEPS, KEEP_TILES, 3, head_t, out_t, keeps, lse).T

    specs_in = (
        P("dp", None), P("dp"), P("tp", None), P(None, "tp"), P(None), P(None), P(None), P(None),
        P(None, "tp"), P(None, "tp"), P(None, "tp"), P("tp", None),
    )
    specs_out = (P("dp", None), P("dp", "tp"))
    return jax.shard_map(draft_step, mesh=mesh, in_specs=specs_in, out_specs=specs_out, check_vma=False)
```

```python
import functools

import jax
import jax.numpy as jnp
from jax import lax
from jax.experimental import pallas as pl
from jax.experimental.pallas import tpu as pltpu
from jax.sharding import PartitionSpec as P

NORM_EPS = 1e-6
SLAB = 8
GROUP = 32
TILE = 1056
HALF = TILE // 2
LANES = 256
KEEPS = 6
KEEP_TILES = 12
CHUNK = 256
LAG = 0
LOWEST = float(jnp.finfo(jnp.float32).min)
F32 = jnp.float32
BF16 = jnp.bfloat16
MESH = pl.DeviceIdType.MESH


def gather_kernel(base_ref, want_ref, table_ref, out_ref, slabs, sems):
    groups = out_ref.shape[0] // GROUP
    span = GROUP * SLAB

    def issue(group, carry):
        for lane in range(GROUP):
            row = group * GROUP + lane
            base = pl.multiple_of(base_ref[row], SLAB)
            pltpu.make_async_copy(
                table_ref.at[pl.ds(base, SLAB), :],
                slabs.at[pl.ds(pl.multiple_of(row * SLAB, SLAB), SLAB), :],
                sems.at[group],
            ).start()
        return carry

    lax.fori_loop(0, groups, issue, 0)

    def select(group, carry):
        block = pl.ds(pl.multiple_of(group * span, span), span)
        rows = pl.ds(pl.multiple_of(group * GROUP, GROUP), GROUP)
        pltpu.make_async_copy(table_ref.at[pl.ds(0, span), :], slabs.at[block, :], sems.at[group]).wait()
        lanes = lax.broadcasted_iota(jnp.int32, (GROUP, span), 1)
        hot = jnp.where(want_ref[rows, :] == lanes, 1.0, 0.0).astype(BF16)
        out_ref[rows, :] = jnp.dot(hot, slabs[block, :], preferred_element_type=F32).astype(BF16)
        return carry

    lax.fori_loop(0, groups, select, 0)


def gather_rows(embedding, local_ids, owned):
    rows, dim = local_ids.shape[0], embedding.shape[1]
    spread = jnp.arange(rows, dtype=jnp.int32)
    ids = jnp.where(owned, local_ids, spread * SLAB % embedding.shape[0])
    place = spread % GROUP
    want = jnp.where(owned, place * SLAB + ids % SLAB, -1)[:, None]
    return pl.pallas_call(
        gather_kernel,
        out_shape=pltpu.VMEM((rows, dim), BF16),
        in_specs=[
            pl.BlockSpec(memory_space=pltpu.SMEM),
            pl.BlockSpec(memory_space=pltpu.VMEM),
            pl.BlockSpec(memory_space=pl.ANY),
        ],
        out_specs=pl.BlockSpec(memory_space=pltpu.VMEM),
        scratch_shapes=[
            pltpu.VMEM((rows * SLAB, dim), BF16),
            pltpu.SemaphoreType.DMA((rows // GROUP,)),
        ],
        compiler_params=pltpu.CompilerParams(vmem_limit_bytes=24 << 20),
        name="gather_rows",
    )(ids // SLAB * SLAB, want, embedding)


def gain_row(gain_ref):
    packed = gain_ref[...]
    return jnp.concatenate([packed[j : j + 1, :] for j in range(packed.shape[0])], axis=1)


def column_of(gain):
    return jnp.broadcast_to(gain, (128, gain.shape[1])).T


def norm_columns(src_ref, dst_ref, gain_ref):
    gain = gain_ref[...]
    dim, tokens = src_ref.shape
    for start in range(0, tokens, 128):
        lanes = pl.ds(start, 128)
        wide = src_ref[:, lanes].astype(F32)
        inv_rms = lax.rsqrt(jnp.sum(wide * wide, axis=0, keepdims=True) / dim + NORM_EPS)
        dst_ref[:, lanes] = (wide * inv_rms * gain).astype(dst_ref.dtype)


def norm_rows(wide, gain):
    inv_rms = lax.rsqrt(jnp.mean(wide * wide, axis=-1, keepdims=True) + NORM_EPS)
    return (wide * inv_rms * gain).astype(BF16)


def mix_kernel(
    n_tp,
    hidden_ref,
    picked_ref,
    h_gain,
    e_gain,
    f_gain,
    o_gain,
    proj_t,
    gate_t,
    up_t,
    down,
    u_full,
    o_ref,
    columns,
    down_t,
    h_normed,
    e_full,
    p_full,
    n_full,
    a_full,
    comb_e,
    pair_e,
    half_e,
    far_e,
    part_d,
    pair_d,
    comb_d,
    half_d,
    far_d,
    send_rs,
    recv_rs,
    send_ag,
    recv_ag,
):
    me = lax.axis_index("tp")
    chips = n_tp // 2
    chip, core = me // 2, me % 2
    partner = chip * 2 + 1 - core
    far = [lax.rem(chip + k, chips) for k in range(chips)]
    back = [lax.rem(chip + chips - k, chips) for k in range(chips)]
    tokens, dim = hidden_ref.shape
    chunks = tokens // CHUNK
    t_rows = CHUNK // n_tp
    f_rows = proj_t.shape[0]
    contract_last = (((1,), (1,)), ((), ()))

    barrier = pltpu.get_barrier_semaphore()
    for peer in [partner] + [far[k] * 2 + core for k in range(1, chips)]:
        pl.semaphore_signal(barrier, inc=1, device_id={"tp": peer}, device_id_type=MESH)
    for start in range(0, tokens, 64):
        rows = pl.ds(start, 64)
        h_normed[rows, :] = norm_rows(hidden_ref[rows, :].astype(F32), gain_row(h_gain))
    columns[0] = column_of(gain_row(f_gain))
    columns[1] = column_of(gain_row(o_gain))
    down_t[...] = down[...].T
    pl.semaphore_wait(barrier, chips)

    def push(src, dst, send_sem, recv_sem, device):
        copy = pltpu.make_async_remote_copy(
            src_ref=src, dst_ref=dst, send_sem=send_sem, recv_sem=recv_sem, device_id={"tp": device}, device_id_type=MESH
        )
        copy.start()
        return copy

    def token_block(chunk):
        return lambda device: (pl.ds(pl.multiple_of(chunk * CHUNK + device * t_rows, 16), t_rows), slice(None))

    def feature_block(chunk):
        return lambda device: (pl.ds(pl.multiple_of(device * f_rows, 16), f_rows), pl.ds(chunk * CHUNK, CHUNK))

    def pair_send(src, block, landing, stage, chunk):
        return [
            push(
                src.at[block(c * 2 + 1 - core)],
                landing.at[chunk, c],
                send_rs.at[stage, chunk, c],
                recv_rs.at[stage, chunk, c],
                partner,
            )
            for c in range(chips)
        ]

    def halves(block):
        rows, lanes = block
        if isinstance(lanes, slice):
            half = t_rows // 2
            return [(pl.ds(pl.multiple_of(rows.start + half * side, 16), half), lanes) for side in range(2)]
        half = CHUNK // 2
        return [(rows, pl.ds(lanes.start + half * side, half)) for side in range(2)]

    def neighbour_halves(shape):
        if shape[0] == t_rows:
            return [(pl.ds(t_rows // 2 * side, t_rows // 2), slice(None)) for side in range(2)]
        return [(slice(None), pl.ds(CHUNK // 2 * side, CHUNK // 2)) for side in range(2)]

    def across_send(sums, landing, stage, chunk):
        parts = neighbour_halves(sums.shape[2:])
        return [
            push(
                sums.at[(chunk, 2) + parts[side]],
                landing.at[chunk, side],
                send_rs.at[stage, chunk, side],
                recv_rs.at[stage, chunk, side],
                far[k] * 2 + core,
            )
            for side, k in ((0, 1), (1, 3))
        ]

    def next_send(sums, across, landing, into, stage, chunk):
        parts = neighbour_halves(sums.shape[2:])
        sends = []
        for side, k in ((0, 1), (1, 3)):
            across[side].wait()
            view = (chunk, k) + parts[side]
            sums[view] = sums[view] + landing[chunk, side]
            sends.append(
                push(
                    sums.at[chunk, k],
                    into.at[chunk, side],
                    send_rs.at[stage, chunk, side],
                    recv_rs.at[stage, chunk, side],
                    far[k] * 2 + core,
                )
            )
        return sends

    def gather_start(full, block, stage, chunk):
        own = full.at[block(me)]
        sends = {
            k: push(own, own, send_ag.at[stage, chunk, k], recv_ag.at[stage, chunk, k], far[k] * 2 + core) for k in (2, 1, 3)
        }
        near = push(own, own, send_ag.at[stage, chunk, 0], recv_ag.at[stage, chunk, 0], partner)
        return sends, near

    def gather_pass(state, full, block, stage, chunk):
        sends, near = state
        passed = []
        for k in [1, 3, 2]:
            sends[k].wait_recv()
            view = full.at[block(back[k] * 2 + core)]
            passed.append(
                push(view, view, send_ag.at[stage, chunk, chips + k], recv_ag.at[stage, chunk, chips + k], partner)
            )
        return [near] + passed, list(sends.values())

    def gather_end(state):
        local, sends = state
        for copy in local:
            copy.wait()
        for copy in sends:
            copy.wait_send()

    live = [None] * chunks

    def e_start(chunk):
        live[chunk] = pair_send(picked_ref, token_block(chunk), pair_e, 0, chunk)

    def e_mid(chunk):
        for copy in live[chunk]:
            copy.wait()
        block, across = token_block(chunk), None
        for k in (2, 1, 3, 0):
            comb_e[chunk, k] = picked_ref[block(far[k] * 2 + core)] + pair_e[chunk, far[k]]
            across = across_send(comb_e, half_e, 1, chunk) if k == 2 else across
        live[chunk] = across

    def e_next(chunk):
        live[chunk] = next_send(comb_e, live[chunk], half_e, far_e, 4, chunk)

    def e_end(chunk):
        total = comb_e[chunk, 0]
        for side in range(2):
            live[chunk][side].wait()
            total = total + far_e[chunk, side]
        block = token_block(chunk)
        e_full[block(me)] = norm_rows(total.astype(F32), gain_row(e_gain))
        live[chunk] = gather_start(e_full, block, 0, chunk)

    def e_pass(chunk):
        live[chunk] = gather_pass(live[chunk], e_full, token_block(chunk), 0, chunk)

    def project(chunk):
        gather_end(live[chunk])
        rows, block = pl.ds(chunk * CHUNK, CHUNK), feature_block(chunk)
        p_own = lax.dot_general(proj_t[:, :dim], h_normed[rows, :], contract_last, preferred_element_type=F32)
        p_own = p_own + lax.dot_general(proj_t[:, dim:], e_full[rows, :], contract_last, preferred_element_type=F32)
        p_full[block(me)] = p_own.astype(BF16)
        live[chunk] = gather_start(p_full, block, 1, chunk)

    def p_pass(chunk):
        live[chunk] = gather_pass(live[chunk], p_full, feature_block(chunk), 1, chunk)

    def feed_forward(chunk):
        gather_end(live[chunk])
        lanes = pl.ds(chunk * CHUNK, CHUNK)
        norm_columns(p_full.at[:, lanes], n_full.at[:, lanes], columns.at[0])
        gate_val = jnp.dot(gate_t[...], n_full[:, lanes], preferred_element_type=F32)
        up_val = jnp.dot(up_t[...], n_full[:, lanes], preferred_element_type=F32)
        a_full[:, lanes] = (gate_val * jax.nn.sigmoid(gate_val) * up_val).astype(BF16)
        part_d[:, lanes] = jnp.dot(down_t[...], a_full[:, lanes], preferred_element_type=F32)
        live[chunk] = pair_send(part_d, feature_block(chunk), pair_d, 2, chunk)

    def d_mid(chunk):
        for copy in live[chunk]:
            copy.wait()
        block, across = feature_block(chunk), None
        for k in (2, 1, 3, 0):
            comb_d[chunk, k] = part_d[block(far[k] * 2 + core)] + pair_d[chunk, far[k]]
            across = across_send(comb_d, half_d, 3, chunk) if k == 2 else across
        live[chunk] = across

    def d_next(chunk):
        live[chunk] = next_send(comb_d, live[chunk], half_d, far_d, 5, chunk)

    def d_end(chunk):
        summed = comb_d[chunk, 0]
        for side in range(2):
            live[chunk][side].wait()
            summed = summed + far_d[chunk, side]
        block = feature_block(chunk)
        u_full[block(me)] = (p_full[block(me)].astype(F32) + summed).astype(BF16)
        live[chunk] = gather_start(u_full, block, 2, chunk)

    def u_pass(chunk):
        live[chunk] = gather_pass(live[chunk], u_full, feature_block(chunk), 2, chunk)

    def finish(chunk):
        gather_end(live[chunk])
        lanes = pl.ds(chunk * CHUNK, CHUNK)
        norm_columns(u_full.at[:, lanes], o_ref.at[:, lanes], columns.at[1])

    stages = (
        e_start, e_mid, e_next, e_end, e_pass, project, p_pass, feed_forward,
        d_mid, d_next, d_end, u_pass, finish,
    )
    turns = sorted((index + LAG * chunk, chunk, index) for index in range(len(stages)) for chunk in range(chunks))
    for _, chunk, index in turns:
        stages[index](chunk)


def mix(n_tp, hidden, picked, gains, proj_w, w_gate, w_up, w_down):
    tokens, dim = hidden.shape
    chips, chunks = n_tp // 2, tokens // CHUNK
    t_rows, f_rows, ffn = CHUNK // n_tp, proj_w.shape[1], w_gate.shape[1]
    vmem = pl.BlockSpec(memory_space=pltpu.VMEM)
    return pl.pallas_call(
        functools.partial(mix_kernel, n_tp),
        out_shape=(pltpu.VMEM((dim, tokens), BF16), pltpu.VMEM((dim, tokens), BF16)),
        in_specs=[vmem] * 10,
        out_specs=(vmem, vmem),
        scratch_shapes=[
            pltpu.VMEM((2, dim, 128), F32),
            pltpu.VMEM((dim, ffn), BF16),
            pltpu.VMEM((tokens, dim), BF16),
            pltpu.VMEM((tokens, dim), BF16),
            pltpu.VMEM((dim, tokens), BF16),
            pltpu.VMEM((dim, tokens), BF16),
            pltpu.VMEM((ffn, tokens), BF16),
            pltpu.VMEM((chunks, chips, t_rows, dim), BF16),
            pltpu.VMEM((chunks, chips, t_rows, dim), BF16),
            pltpu.VMEM((chunks, 2, t_rows // 2, dim), BF16),
            pltpu.VMEM((chunks, 2, t_rows, dim), BF16),
            pltpu.VMEM((dim, tokens), F32),
            pltpu.VMEM((chunks, chips, f_rows, CHUNK), F32),
            pltpu.VMEM((chunks, chips, f_rows, CHUNK), F32),
            pltpu.VMEM((chunks, 2, f_rows, CHUNK // 2), F32),
            pltpu.VMEM((chunks, 2, f_rows, CHUNK), F32),
            pltpu.SemaphoreType.DMA((6, chunks, chips)),
            pltpu.SemaphoreType.DMA((6, chunks, chips)),
            pltpu.SemaphoreType.DMA((3, chunks, 10)),
            pltpu.SemaphoreType.DMA((3, chunks, 10)),
        ],
        compiler_params=pltpu.CompilerParams(collective_id=0, has_side_effects=True, vmem_limit_bytes=32 << 20),
        name="mix",
    )(*[pltpu.with_memory_space_constraint(x, pltpu.VMEM) for x in (hidden, picked, *gains, proj_w.T, w_gate.T, w_up.T, w_down)])


def stats_kernel(n_tp, n_keep, keep_tiles, head_ref, o_ref, lse_ref, *refs):
    keeps = refs[:n_keep]
    max_ref, sum_ref, slots, held, base, mine, theirs, sems, send_sem, recv_sem = refs[n_keep:]
    me = lax.axis_index("tp")
    peers = [lax.rem(me + k, n_tp) for k in range(1, n_tp)]
    barrier = pltpu.get_barrier_semaphore()
    for peer in peers:
        pl.semaphore_signal(barrier, inc=1, device_id={"tp": peer}, device_id_type=MESH)
    each = keep_tiles // n_keep
    vocab, tokens = head_ref.shape[0], o_ref.shape[1]
    full, tail = vocab // TILE, vocab % TILE
    depth = slots.shape[0]

    def fetch(tile, rows):
        slot = lax.rem(tile, depth)
        return pltpu.make_async_copy(
            head_ref.at[pl.ds(pl.multiple_of(tile * TILE, 16), rows), :],
            slots.at[slot, pl.ds(0, rows), :],
            sems.at[slot],
        )

    def fetch_any(tile):
        @pl.when(tile < full)
        def _():
            fetch(tile, TILE).start()

        if tail:

            @pl.when(tile == full)
            def _():
                fetch(tile, tail).start()

    def parts(rows):
        return [(0, rows)]

    def groups(z):
        return z.reshape(z.shape[0] // 8, 8, z.shape[1])

    def rescale(lanes):
        top = max_ref[:, lanes]
        sum_ref[:, lanes] = sum_ref[:, lanes] * jnp.exp(base[:, lanes] - top)
        base[:, lanes] = top

    def add_held(top, size, lanes):
        z = groups(held[pl.ds(top, size), lanes])
        sum_ref[:, lanes] = sum_ref[:, lanes] + jnp.sum(jnp.exp(z - base[:, lanes][None]), axis=0)

    def work(tile, rows, keep):
        slot = lax.rem(tile, depth)
        for start in range(0, tokens, LANES):
            lanes = pl.ds(start, LANES)
            rescale(lanes)
            for top, size in parts(TILE):
                add_held(top, size, lanes)
                size = min(size, rows - top)
                z = jnp.dot(slots[slot, pl.ds(top, size), :], o_ref[:, lanes], preferred_element_type=F32)
                if keep is not None:
                    keeps[keep][pl.ds(pl.multiple_of((tile - keep * each) * TILE + top, 16), size), lanes] = z
                held[pl.ds(top, size), lanes] = z
                max_ref[:, lanes] = jnp.maximum(max_ref[:, lanes], jnp.max(groups(z), axis=0))

    for tile in range(depth - 1):
        fetch(tile, TILE).start()
    max_ref[...] = jnp.full_like(max_ref, LOWEST)
    base[...] = jnp.full_like(base, LOWEST)
    sum_ref[...] = jnp.zeros_like(sum_ref)
    held[...] = jnp.full_like(held, -jnp.inf)

    def step(keep, tile, carry):
        fetch_any(tile + depth - 1)
        fetch(tile, TILE).wait()
        work(tile, TILE, keep)
        return carry

    for index in range(n_keep):
        lax.fori_loop(index * each, (index + 1) * each, functools.partial(step, index), 0)
    lax.fori_loop(keep_tiles, full, functools.partial(step, None), 0)
    if tail:
        fetch(full, tail).wait()
        work(full, tail, None)
    for start in range(0, tokens, LANES):
        rescale(pl.ds(start, LANES))
        for top, size in parts(tail or TILE):
            add_held(top, size, pl.ds(start, LANES))

    best = jnp.max(max_ref[...], axis=0, keepdims=True)
    total = jnp.sum(sum_ref[...] * jnp.exp(max_ref[...] - best), axis=0, keepdims=True)
    mine[...] = jnp.concatenate([best, total], axis=0)
    pl.semaphore_wait(barrier, n_tp - 1)
    copies = []
    for k, peer in enumerate(peers):
        copy = pltpu.make_async_remote_copy(
            src_ref=mine,
            dst_ref=theirs.at[k],
            send_sem=send_sem.at[k],
            recv_sem=recv_sem.at[k],
            device_id={"tp": peer},
            device_id_type=MESH,
        )
        copy.start()
        copies.append(copy)
    for k, copy in enumerate(copies):
        copy.wait()
        arrived = theirs[k]
        other, extra = arrived[0:1, :], arrived[1:2, :]
        new = jnp.maximum(best, other)
        total = total * jnp.exp(best - new) + extra * jnp.exp(other - new)
        best = new
    lse_ref[...] = jnp.broadcast_to(best + jnp.log(total), lse_ref.shape)


def head_stats(n_tp, n_keep, keep_tiles, depth, head_t, o_t):
    vocab, dim = head_t.shape
    tokens = o_t.shape[1]
    vmem = pl.BlockSpec(memory_space=pltpu.VMEM)
    return pl.pallas_call(
        functools.partial(stats_kernel, n_tp, n_keep, keep_tiles),
        out_shape=(
            jax.ShapeDtypeStruct((8, tokens), F32),
            *[pltpu.VMEM((keep_tiles // n_keep * TILE, tokens), F32)] * n_keep,
        ),
        in_specs=[pl.BlockSpec(memory_space=pl.ANY), vmem],
        out_specs=(vmem,) * (n_keep + 1),
        scratch_shapes=[
            pltpu.VMEM((8, tokens), F32),
            pltpu.VMEM((8, tokens), F32),
            pltpu.VMEM((depth, TILE, dim), BF16),
            pltpu.VMEM((TILE, tokens), F32),
            pltpu.VMEM((8, tokens), F32),
            pltpu.VMEM((2, tokens), F32),
            pltpu.VMEM((n_tp - 1, 2, tokens), F32),
            pltpu.SemaphoreType.DMA((depth,)),
            pltpu.SemaphoreType.DMA((n_tp - 1,)),
            pltpu.SemaphoreType.DMA((n_tp - 1,)),
        ],
        compiler_params=pltpu.CompilerParams(collective_id=1, has_side_effects=True, vmem_limit_bytes=12 << 20),
        name="head_stats",
    )(pltpu.with_memory_space_constraint(head_t, pltpu.HBM), pltpu.with_memory_space_constraint(o_t, pltpu.VMEM))


def logp_kernel(n_keep, keep_tiles, head_ref, o_ref, u_t, lse_ref, *refs):
    keeps = refs[:n_keep]
    out_ref, u_ref, slots, made, kept, u_rows, in_sems, made_sems, kept_sems, u_sem = refs[n_keep:]
    vocab, tokens = head_ref.shape[0], o_ref.shape[1]
    each = keep_tiles // n_keep * 2
    kept_chunks = keep_tiles * 2
    base = keep_tiles * TILE
    rest = vocab - base
    steps, tail = rest // HALF, rest % HALF
    n_slots = kept.shape[0]
    spans = [steps * (i + 1) // n_keep for i in range(n_keep)]

    def fetch(step, rows):
        slot = lax.rem(step, 2)
        return pltpu.make_async_copy(
            head_ref.at[pl.ds(pl.multiple_of(base + step * HALF, 16), rows), :], slots.at[slot, pl.ds(0, rows), :], in_sems.at[slot])

    def put_made(step, rows):
        slot = lax.rem(step, 2)
        return pltpu.make_async_copy(
            made.at[slot, pl.ds(0, rows), :], out_ref.at[pl.ds(pl.multiple_of(base + step * HALF, 16), rows), :], made_sems.at[slot])

    def put_kept(chunk):
        slot = lax.rem(chunk, n_slots)
        return pltpu.make_async_copy(
            kept.at[slot], out_ref.at[pl.ds(pl.multiple_of(chunk * HALF, 16), HALF), :], kept_sems.at[slot])

    def do_kept(index, chunk):
        @pl.when(chunk >= n_slots)
        def _():
            put_kept(chunk - n_slots).wait()
        slot = lax.rem(chunk, n_slots)
        rows = pl.ds(pl.multiple_of((chunk - index * each) * HALF, 16), HALF)
        for start in range(0, tokens, LANES):
            lanes = pl.ds(start, LANES)
            kept[slot, :, lanes] = keeps[index][rows, lanes] - lse_ref[:, lanes][0:1, :]
        put_kept(chunk).start()

    def make(step, rows):
        slot = lax.rem(step, 2)
        for start in range(0, tokens, LANES):
            lanes = pl.ds(start, LANES)
            z = jnp.dot(slots[slot, pl.ds(0, rows), :], o_ref[:, lanes], preferred_element_type=F32)
            made[slot, pl.ds(0, rows), lanes] = z - lse_ref[:, lanes][0:1, :]

    def start_fetch(step):
        @pl.when(step < steps)
        def _():
            fetch(step, HALF).start()
        if tail:
            @pl.when(step == steps)
            def _():
                fetch(step, tail).start()

    start_fetch(0)
    u_copy = pltpu.make_async_copy(u_rows, u_ref, u_sem)
    done_steps = 0
    for index in range(n_keep):
        stop = spans[index]
        count = stop - done_steps
        per_step = each // count if count else 0

        def step_fn(step, carry, index=index, first=done_steps, per_step=per_step):
            start_fetch(step + 1)
            for i in range(per_step):
                do_kept(index, index * each + (step - first) * per_step + i)
            fetch(step, HALF).wait()
            @pl.when(step >= 2)
            def _():
                put_made(step - 2, HALF).wait()
            make(step, HALF)
            put_made(step, HALF).start()
            return carry

        lax.fori_loop(done_steps, stop, step_fn, 0)

        def kept_fn(chunk, carry, index=index):
            do_kept(index, chunk)
            return carry
        lax.fori_loop(index * each + count * per_step, (index + 1) * each, kept_fn, 0)
        if index < tokens // 256:
            for start in range(index * 256, (index + 1) * 256, 128):
                u_rows[pl.ds(start, 128), :] = u_t[:, pl.ds(start, 128)].T
        done_steps = stop
    u_copy.start()
    if tail:
        fetch(steps, tail).wait()
        put_made(steps - 2, HALF).wait()
        make(steps, tail)
        put_made(steps, tail).start()
        put_made(steps - 1, HALF).wait()
        put_made(steps, tail).wait()
    else:
        put_made(steps - 2, HALF).wait()
        put_made(steps - 1, HALF).wait()
    for i in range(n_slots):
        put_kept(kept_chunks - n_slots + i).wait()
    u_copy.wait()

def head_logp(n_keep, keep_tiles, n_kept, head_t, o_t, u_t, keeps, lse):
    vocab, dim = head_t.shape
    tokens = o_t.shape[1]
    vmem = pl.BlockSpec(memory_space=pltpu.VMEM)
    anym = pl.BlockSpec(memory_space=pl.ANY)
    return pl.pallas_call(
        functools.partial(logp_kernel, n_keep, keep_tiles),
        out_shape=(jax.ShapeDtypeStruct((vocab, tokens), F32), jax.ShapeDtypeStruct((tokens, dim), BF16)),
        in_specs=[anym] + [vmem] * (n_keep + 3),
        out_specs=(anym, anym),
        scratch_shapes=[
            pltpu.VMEM((2, HALF, dim), BF16),
            pltpu.VMEM((2, HALF, tokens), F32),
            pltpu.VMEM((n_kept, HALF, tokens), F32),
            pltpu.VMEM((tokens, dim), BF16),
            pltpu.SemaphoreType.DMA((2,)), pltpu.SemaphoreType.DMA((2,)), pltpu.SemaphoreType.DMA((n_kept,)), pltpu.SemaphoreType.DMA,
        ],
        compiler_params=pltpu.CompilerParams(vmem_limit_bytes=16 << 20),
        name="head_logp",
    )(pltpu.with_memory_space_constraint(head_t, pltpu.HBM), pltpu.with_memory_space_constraint(o_t, pltpu.VMEM), pltpu.with_memory_space_constraint(u_t, pltpu.VMEM), lse, *[pltpu.with_memory_space_constraint(keep, pltpu.VMEM) for keep in keeps])


def solution(mesh):
    n_tp = mesh.shape["tp"]

    def draft_step(hidden, tokens, embedding, head_w, h_norm, e_norm, f_norm, o_norm, proj_w, w_gate, w_up, w_down):
        vocab_local = embedding.shape[0]
        local_ids = tokens - lax.axis_index("tp") * vocab_local
        owned = (local_ids >= 0) & (local_ids < vocab_local)
        picked = gather_rows(embedding, local_ids, owned)
        gains = [gain.reshape(-1, 128) for gain in (h_norm, e_norm, f_norm, o_norm)]
        u_t, out_t = mix(n_tp, hidden, picked, gains, proj_w, w_gate, w_up, w_down)
        head_t = head_w.T
        lse, *keeps = head_stats(n_tp, KEEPS, KEEP_TILES, 3, head_t, out_t)
        logp_t, new_u = head_logp(KEEPS, KEEP_TILES, 3, head_t, out_t, u_t, keeps, lse)
        return new_u, logp_t.T

    specs_in = (
        P("dp", None), P("dp"), P("tp", None), P(None, "tp"), P(None), P(None), P(None), P(None),
        P(None, "tp"), P(None, "tp"), P(None, "tp"), P("tp", None),
    )
    specs_out = (P("dp", None), P("dp", "tp"))
    return jax.shard_map(draft_step, mesh=mesh, in_specs=specs_in, out_specs=specs_out, check_vma=False)
```
